32 devices in a mesh: gx: 2 (over x), gy: 4 (over z), gz: 4 (over y, core).
Axes of the slice: x: 2, y: 2, z: 4, core: 2. Of those that a mesh axis runs over, the one named last changes fastest.
Arguments:
- source_points: float32 [1024, 3, 384], P(('gx', 'gy', 'gz'))
- target_points: float32 [1024, 3, 384], P(('gx', 'gy', 'gz'))
- pair_scans: int32 [1024, 2], P(('gx', 'gy', 'gz')), may hold values from 0 to 127, as said below
- point_counts: int32 [1024, 2], P(('gx', 'gy', 'gz')), may hold values from 48 to 384
- live_tasks: int32 [32], P(('gx', 'gy', 'gz')), may hold values from 1 to 32, as said below
- pose_init: float32 [128, 12], P(('gx', 'gy', 'gz')), may hold values from -1 to 1, as said below
- gauge: int32 [1], replicated, may hold values from 0 to 127
Outputs:
- poses_out: float32 [128, 12], P(('gx', 'gy', 'gz'))
The draws below stay inside these ranges and needn't reach their ends.
Inputs may be any that keep to these rules, and one draw needn't show every extreme that they name: pair_scans[p, 0] is one of the 4 scans of the device that holds slot p (scans are numbered 4 a device, in device order); pair_scans[p, 1] differs from pair_scans[p, 0]. `live_tasks`: the live slots of a device are its first ones; some device has 32 live slots. `pose_init`: each rotation is orthonormal.
All inputs are finite; a program needn't handle non-finite values.
Results may differ from the reference program's by a relative error of at most 0.0003.
Values sent between devices are 32-bit elements; how exact they have to be, the bound alone decides.
No kernel may reach another device: no remote copies, remote signals or barrier semaphores. Data moves between devices by JAX's collectives and lax.ppermute only.
A program may use at most 64 MiB of HBM per device.

```python
import jax
import jax.numpy as jnp
from jax import lax

P_SIZE = 384
TASK_DEV = 32
SCAN_DEV = 4
ITERS = 2
HOMES = 32
SCANS = 128
PAIRS = 1024


def point_cloud(key):
    base_key = jax.random.fold_in(key, 11)
    keys = jax.random.split(base_key, 3)
    base = 2.0 * jax.random.normal(keys[0], (PAIRS, 3, P_SIZE), jnp.float32)
    source = base + 0.15 * jax.random.normal(keys[1], (PAIRS, 3, P_SIZE), jnp.float32)
    target = base + 0.15 * jax.random.normal(keys[2], (PAIRS, 3, P_SIZE), jnp.float32)
    return (source, target)


def draw_source_points(key, part):
    return point_cloud(key)[0]


def draw_target_points(key, part):
    return point_cloud(key)[1]


def draw_pair_scans(key, part):
    keys = jax.random.split(jax.random.fold_in(key, 23), 2)
    owners = jnp.arange(PAIRS, dtype=jnp.int32) // TASK_DEV * SCAN_DEV
    first_scan = owners + jax.random.randint(keys[0], (PAIRS,), 0, SCAN_DEV, dtype=jnp.int32)
    second_scan = (first_scan + jax.random.randint(keys[1], (PAIRS,), 1, SCANS, dtype=jnp.int32)) % SCANS
    return jnp.stack([first_scan, second_scan], axis=1).astype(jnp.int32)


def draw_live_tasks(key, part):
    keys = jax.random.split(jax.random.fold_in(key, 37), 3)
    first_factor = jax.random.randint(keys[0], (HOMES,), 0, TASK_DEV, dtype=jnp.int32)
    second_factor = jax.random.randint(keys[1], (HOMES,), 0, TASK_DEV, dtype=jnp.int32)
    counts = 1 + first_factor * second_factor // TASK_DEV
    busiest = jax.random.randint(keys[2], (), 0, HOMES, dtype=jnp.int32)
    return counts.at[busiest].set(TASK_DEV).astype(jnp.int32)


def draw_pose_init(key, part):
    keys = jax.random.split(jax.random.fold_in(key, 41), 2)
    angles = 0.03 * jax.random.normal(keys[0], (SCANS, 3), jnp.float32)
    shifts = 0.1 * jax.random.normal(keys[1], (SCANS, 3), jnp.float32)
    half_angle = 0.5 * angles
    zeros_col = jnp.zeros_like(half_angle[:, 0])
    first, second, third = (half_angle[:, 0], half_angle[:, 1], half_angle[:, 2])
    cross_mat = jnp.stack([jnp.stack([zeros_col, -third, second], 1), jnp.stack([third, zeros_col, -first], 1), jnp.stack([-second, first, zeros_col], 1)], 1)
    half_norm = jnp.sum(half_angle * half_angle, axis=1)
    rotation = jnp.eye(3, dtype=jnp.float32) + (2.0 / (1.0 + half_norm))[:, None, None] * (cross_mat + jnp.einsum('nij,njk->nik', cross_mat, cross_mat))
    return jnp.concatenate([rotation.reshape(SCANS, 9), shifts], axis=1).astype(jnp.float32)


def with_ends(entries, rng, low, high):
    place = [jax.random.randint(jax.random.fold_in(rng, axis), (), 0, length) for axis, length in enumerate(entries.shape)]
    longest = entries.shape.index(max(entries.shape))
    beside = place[:longest] + [(place[longest] + 1) % entries.shape[longest]] + place[longest + 1:]
    return entries.at[tuple(place)].set(low).at[tuple(beside)].set(high)


def setup_inputs(seed: int = 0) -> dict:
    key_list = jax.random.split(jax.random.key(seed), 8)
    return {
        "source_points": draw_source_points(jax.random.fold_in(key_list[7], 71), 0),
        "target_points": draw_target_points(jax.random.fold_in(key_list[7], 71), 0),
        "pair_scans": draw_pair_scans(jax.random.fold_in(key_list[7], 71), 0),
        "point_counts": with_ends(jax.random.randint(key_list[3], (PAIRS, 2), P_SIZE // 8, P_SIZE + 1), jax.random.fold_in(key_list[3], 1), P_SIZE // 8, P_SIZE).astype(jnp.int32),
        "live_tasks": draw_live_tasks(jax.random.fold_in(key_list[7], 71), 0),
        "pose_init": draw_pose_init(jax.random.fold_in(key_list[7], 71), 0),
        "gauge": jax.random.randint(key_list[6], (1,), 0, SCANS).astype(jnp.int32),
    }


INV_SPREAD = 2.0
DAMPING = 1.0
FLOOR_SCORE = -1e30


def transform(pose, points):
    rotation = pose[:9].reshape(3, 3)
    return jnp.dot(rotation, points, precision=lax.Precision.HIGHEST) + pose[9:, None]


def jacobian(points):
    zeros_row = jnp.zeros_like(points[0])
    ones_row = jnp.ones_like(points[0])
    first, second, third = points[0], points[1], points[2]
    row_one = jnp.stack([zeros_row, third, -second, ones_row, zeros_row, zeros_row])
    row_two = jnp.stack([-third, zeros_row, first, zeros_row, ones_row, zeros_row])
    row_three = jnp.stack([second, -first, zeros_row, zeros_row, zeros_row, ones_row])
    return jnp.stack([row_one, row_two, row_three])


def normal_terms(derivative, residual, weight):
    hessian = jnp.einsum("kap,kbp,p->ab", derivative, derivative, weight, precision=lax.Precision.HIGHEST)
    gradient = jnp.einsum("kap,kp,p->a", derivative, residual, weight, precision=lax.Precision.HIGHEST)
    return jnp.concatenate([hessian.reshape(36), gradient])


def pair_terms(source, target, counts, pose_a, pose_b, live):
    width = source.shape[1]
    moved_x = transform(pose_a, source)
    moved_y = transform(pose_b, target)
    positions = jnp.arange(width, dtype=jnp.int32)
    differ = moved_x[:, :, None] - moved_y[:, None, :]
    distance = jnp.sum(differ * differ, axis=0)
    score = jnp.where(positions[None, :] < counts[1], -INV_SPREAD * distance, FLOOR_SCORE)
    weights = jax.nn.softmax(score, axis=1)
    matched = jnp.dot(moved_y, weights.T, precision=lax.Precision.HIGHEST)
    residual = moved_x - matched
    weight = jnp.where(positions < counts[0], 1.0, 0.0).astype(jnp.float32) * live
    return normal_terms(jacobian(moved_x), residual, weight), normal_terms(jacobian(matched), -residual, weight)


def spd_solve(matrix, rhs):
    augmented = jnp.concatenate([matrix, rhs[:, :, None]], axis=2)
    for column in range(6):
        pivot_row = augmented[:, column, :] / augmented[:, column, column:column + 1]
        augmented = augmented - augmented[:, :, column:column + 1] * pivot_row[:, None, :]
        augmented = augmented.at[:, column, :].set(pivot_row)
    return augmented[:, :, 6]


def cross_matrix(vector):
    zeros_col = jnp.zeros_like(vector[:, 0])
    first, second, third = vector[:, 0], vector[:, 1], vector[:, 2]
    return jnp.stack([jnp.stack([zeros_col, -third, second], 1), jnp.stack([third, zeros_col, -first], 1), jnp.stack([-second, first, zeros_col], 1)], 1)


def update(poses, totals, fixed):
    hessian = totals[:, :36].reshape(-1, 6, 6) + DAMPING * jnp.eye(6, dtype=jnp.float32)
    gradient = totals[:, 36:]
    increment = -spd_solve(hessian, gradient)
    increment = jnp.where(fixed[:, None], 0.0, increment)
    half_angle = increment[:, :3] * 0.5
    half_norm = jnp.sum(half_angle * half_angle, axis=1)
    cross_mat = cross_matrix(half_angle)
    square = jnp.einsum("nij,njk->nik", cross_mat, cross_mat, precision=lax.Precision.HIGHEST)
    rotation_step = jnp.eye(3, dtype=jnp.float32) + (2.0 / (1.0 + half_norm))[:, None, None] * (cross_mat + square)
    rotation = poses[:, :9].reshape(-1, 3, 3)
    new_rotation = jnp.einsum("nij,njk->nik", rotation_step, rotation, precision=lax.Precision.HIGHEST)
    new_shift = jnp.einsum("nij,nj->ni", rotation_step, poses[:, 9:], precision=lax.Precision.HIGHEST) + increment[:, 3:]
    return jnp.concatenate([new_rotation.reshape(-1, 9), new_shift], axis=1)


def reference(source_points, target_points, pair_scans, point_counts, live_tasks, pose_init, gauge):
    slots = jnp.arange(PAIRS, dtype=jnp.int32)
    live_flag = ((slots % TASK_DEV) < jnp.repeat(live_tasks, TASK_DEV)).astype(jnp.float32)
    fixed = jnp.arange(SCANS, dtype=jnp.int32) == gauge[0]
    poses = pose_init
    for iteration in range(ITERS):
        pose_a = poses[pair_scans[:, 0]]
        pose_b = poses[pair_scans[:, 1]]

        def one_pair(items):
            return pair_terms(*items)

        terms_a, terms_b = lax.map(one_pair, (source_points, target_points, point_counts, pose_a, pose_b, live_flag))
        totals = jax.ops.segment_sum(terms_a, pair_scans[:, 0], SCANS) + jax.ops.segment_sum(terms_b, pair_scans[:, 1], SCANS)
        poses = update(poses, totals, fixed)
    return poses
```

```python
import jax
import jax.numpy as jnp
from jax import lax
from jax.experimental import pallas as pl
from jax.experimental.pallas import tpu as pltpu
from jax.sharding import PartitionSpec as P

AXES = ("gx", "gy", "gz")
ITERS = 2
SPREAD = 2.0
DAMPING = 1.0
FLOOR = -1e30
LOG2E = 1.4426950408889634
LIFT = 100.0
TINY = 2.0**-100
UNROLL = 8
STEP = 8
SCALE = 2.0 * SPREAD * LOG2E
LANES = 128


def halves(value):
    first = value.astype(jnp.bfloat16).astype(jnp.float32)
    rest = value - first
    second = rest.astype(jnp.bfloat16).astype(jnp.float32)
    return first, second, rest - second


def moved(points_ref, task, pose, row3, width):
    reps = width // LANES

    def column(index):
        a, b, c = (pose(index, r) for r in range(3))
        col = jnp.where(row3 == 0, a, jnp.where(row3 == 1, b, c))
        return jnp.concatenate([col] * reps, axis=1)

    out = column(3)
    for axis in range(3):
        row = jnp.broadcast_to(points_ref[axis, pl.ds(task, 1), :], (8, width))
        out = out + column(axis) * row
    return out


def operands(task, pose_of, ids_ref, counts_ref, src_ref, tgt_ref):
    width = src_ref.shape[2]
    sub = lax.broadcasted_iota(jnp.int32, (8, LANES), 0)
    row3 = sub - 3 * (sub // 3)
    row = lax.broadcasted_iota(jnp.int32, (8, width), 0)
    lane = lax.broadcasted_iota(jnp.int32, (8, width), 1)
    pos_x = moved(src_ref, task, pose_of(ids_ref[0, task]), row3, width)
    pos_y = moved(tgt_ref, task, pose_of(ids_ref[1, task]), row3, width)
    sq_x = pos_x * pos_x
    norm_x = pltpu.roll(sq_x, 1, 0) + pltpu.roll(sq_x, 2, 0) + pltpu.roll(sq_x, 3, 0)
    base_x = jnp.where(row < 6, pos_x, jnp.where(row == 6, LIFT - SPREAD * LOG2E * norm_x, 1.0))
    sq_y = pos_y * pos_y
    norm_y = pltpu.roll(sq_y, 2, 0) + pltpu.roll(sq_y, 3, 0) + pltpu.roll(sq_y, 4, 0)
    last_y = jnp.where(lane < counts_ref[1, task], -SPREAD * LOG2E * norm_y, FLOOR)
    base_y = jnp.where(row < 6, SCALE * pos_y, jnp.where(row == 6, 1.0, last_y))
    x_one, x_two, x_three = halves(base_x)
    y_one, y_two, y_three = halves(base_y)
    low3 = row < 3
    mid3 = (row >= 3) & (row < 6)
    x_group = [
        x_one,
        jnp.where(low3 | (row == 7), x_one, x_three),
        jnp.where(row == 7, x_one, x_two),
    ]
    y_group = [
        jnp.where(mid3, y_two, y_one),
        jnp.where(low3 | (row == 7), y_three, y_one),
        jnp.where(low3 | (row == 6), y_one, y_two),
    ]
    blank = jnp.zeros((8, width), jnp.float32)
    mat_x = jnp.concatenate(x_group + [blank], axis=0).astype(jnp.bfloat16)
    mat_y = jnp.concatenate(y_group + [blank], axis=0).astype(jnp.bfloat16)
    return pos_x, mat_x, mat_y


def score_of(turned_y, mat_x):
    return jnp.dot(turned_y, mat_x, preferred_element_type=jnp.float32)


def pull_sums(mat_y, weight):
    return jnp.dot(mat_y, weight.astype(jnp.bfloat16), preferred_element_type=jnp.float32)


def moments(task, live, counts_ref, pos_x, sums, acc_ref, low_ref):
    width = pos_x.shape[1]
    row = lax.broadcasted_iota(jnp.int32, (8, width), 0)
    lane = lax.broadcasted_iota(jnp.int32, (8, width), 1)
    count_x = jnp.where(task < live, counts_ref[0, task], 0)
    top = sums[:8]
    bottom = sums[8:]
    total = top[6:7, :]
    valid = lane < count_x
    low3 = row < 3
    low_ref[...] = jnp.minimum(low_ref[...], jnp.where(valid[:1], total, 1.0))
    inverse = jnp.broadcast_to((1.0 / SCALE) / total, (8, width))
    match_mid = (top + bottom + pltpu.roll(bottom, 3, 0)) * inverse
    match = jnp.where(valid, jnp.where(low3, pltpu.roll(match_mid, 5, 0), match_mid), 0.0)
    pos = jnp.where(valid, pos_x, 0.0)
    diff = pos - match
    next_pos = pltpu.roll(pos, 7, 0)
    ones = jnp.where(valid & (row == 6), 1.0, 0.0)
    linear = jnp.where(low3, pos, jnp.where(row < 6, match, ones))
    turned = jnp.where(low3, next_pos, pltpu.roll(match, 2, 0))
    cross = pos * pltpu.roll(diff, 7, 0) - next_pos * diff
    tail = jnp.where(low3, cross, diff)
    acc_lane = lax.broadcasted_iota(jnp.int32, (8, LANES), 1)
    for slot, part in enumerate((linear, linear * linear, linear * turned, tail)):
        reduced = jnp.sum(part, axis=1, keepdims=True)
        span = pl.ds(8 * slot, 8)
        acc_ref[span, :] = jnp.where(acc_lane == task, reduced, acc_ref[span, :])


def all_tasks(pose_of, data, work):
    live_ref, ids_ref, counts_ref, src_ref, tgt_ref = data
    acc_ref, low_ref, pos_ref, mx_ref, my_ref, mt_ref, sums_ref, even_ref, odd_ref, items_ref = work
    tasks = src_ref.shape[1]
    width = src_ref.shape[2]
    chunks = width // LANES
    live = live_ref[0]
    acc_ref[...] = jnp.zeros_like(acc_ref)
    low_ref[...] = jnp.ones_like(low_ref)
    mx_ref[tasks] = jnp.zeros_like(mx_ref[tasks])
    for chunk in range(chunks):
        my_ref[tasks * chunks + chunk] = jnp.zeros_like(my_ref[0])
        mt_ref[tasks * chunks + chunk] = jnp.zeros_like(mt_ref[0])
    unroll = UNROLL if tasks % UNROLL == 0 else 1
    groups = (live + unroll - 1) // unroll
    def prepare(group, end):
        for inner in range(unroll):
            task = group * unroll + inner
            pos_x, mat_x, mat_y = operands(task, pose_of, ids_ref, counts_ref, src_ref, tgt_ref)
            pos_ref[task] = pos_x
            mx_ref[task] = mat_x
            for chunk in range(chunks):
                block = mat_y[:, chunk * LANES : (chunk + 1) * LANES]
                my_ref[task * chunks + chunk] = block[:16]
                mt_ref[task * chunks + chunk] = block.T
            for chunk in range(chunks):
                items_ref[end + chunk] = task * chunks + chunk
            used = (counts_ref[1, task] + LANES - 1) // LANES
            end = end + jnp.where(task < live, used, 0)
        return end

    count = lax.fori_loop(0, groups, prepare, jnp.int32(0))
    for pad in range(3 * STEP):
        items_ref[count + pad] = tasks * chunks
    rounds = (count + STEP - 1) // STEP

    def score(index, buffer_ref, slot):
        code = items_ref[index]
        score = score_of(mt_ref[code], mx_ref[code // chunks])
        buffer_ref[slot] = jnp.exp2(score).astype(jnp.bfloat16)

    def pull(index, buffer_ref, slot):
        code = items_ref[index]
        task = code // chunks
        out = pull_sums(my_ref[code], buffer_ref[slot])
        prior = jnp.where(code == task * chunks, 0.0, sums_ref[task])
        sums_ref[task] = prior + out

    def both(group, next_ref, this_ref):
        for slot in range(STEP):
            score((group + 1) * STEP + slot, next_ref, slot)
            pull(group * STEP + slot, this_ref, slot)

    for slot in range(STEP):
        score(slot, even_ref, slot)

    def pair(index, carry):
        both(2 * index, odd_ref, even_ref)

        @pl.when(2 * index + 1 < rounds)
        def _():
            both(2 * index + 1, even_ref, odd_ref)

        return carry

    lax.fori_loop(0, (rounds + 1) // 2, pair, 0)

    def finish(group, carry):
        for inner in range(unroll):
            task = group * unroll + inner
            moments(task, live, counts_ref, pos_ref[task], sums_ref[task], acc_ref, low_ref)
        return carry

    lax.fori_loop(0, groups, finish, 0)

    @pl.when(jnp.min(low_ref[...]) < TINY)
    def _():
        def again(task, carry):
            pos_x, mat_x, mat_y = operands(task, pose_of, ids_ref, counts_ref, src_ref, tgt_ref)
            score = score_of(mat_y.T, mat_x)
            weight = jnp.exp2(score - jnp.max(score, axis=0, keepdims=True))
            moments(task, live, counts_ref, pos_x, pull_sums(mat_y[:16], weight), acc_ref, low_ref)
            return carry

        lax.fori_loop(0, live, again, 0)


def scatter(acc_ref, pairs_ref, scans):
    row_id = lax.broadcasted_iota(jnp.int32, (scans, LANES), 0)
    parts = jnp.concatenate(halves(acc_ref[...]), axis=0).astype(jnp.bfloat16)

    def side(index):
        hot = (pairs_ref[index : index + 1, :] == row_id).astype(jnp.float32).astype(jnp.bfloat16)
        out = lax.dot_general(
            parts, hot, (((1,), (1,)), ((), ())), preferred_element_type=jnp.float32
        )
        return out[:32] + (out[32:64] + out[64:])

    sum_a = side(0)
    sum_b = side(1)
    row = lax.broadcasted_iota(jnp.int32, (8, scans), 0)

    def low(slot):
        span = slice(8 * slot, 8 * slot + 8)
        return sum_a[span] + pltpu.roll(sum_b[span], 5, 0)

    count = sum_a[:8] + sum_b[:8]
    mixed = low(2)
    tail = sum_a[24:] - sum_b[24:]
    first = jnp.where(row < 3, low(0), pltpu.roll(low(1), 3, 0))
    first = jnp.where(row < 6, first, jnp.where(row == 6, count, pltpu.roll(mixed, 7, 0)))
    second = jnp.where(row < 6, tail, pltpu.roll(mixed, 5, 0))
    return first, second


def updated(first, second, pose_rows, fixed):
    def cross(a, b):
        return (
            a[1] * b[2] - a[2] * b[1],
            a[2] * b[0] - a[0] * b[2],
            a[0] * b[1] - a[1] * b[0],
        )

    at = lambda arr, index: arr[index : index + 1, :]
    lin = [at(first, k) for k in range(3)]
    xx, yy, zz = (at(first, 3 + k) for k in range(3))
    mass = at(first, 6) + DAMPING
    xy = at(first, 7)
    yz = at(second, 6)
    zx = at(second, 7)
    turn = [at(second, 1), at(second, 2), at(second, 0)]
    pull = [at(second, 3 + k) for k in range(3)]
    inverse = 1.0 / mass
    sx, sy, sz = lin
    ux, uy, uz = sx * inverse, sy * inverse, sz * inverse
    h00 = (yy + zz) + DAMPING - (sy * uy + sz * uz)
    h11 = (xx + zz) + DAMPING - (sx * ux + sz * uz)
    h22 = (xx + yy) + DAMPING - (sx * ux + sy * uy)
    h01 = sx * uy - xy
    h02 = sx * uz - zx
    h12 = sy * uz - yz
    lever = cross((ux, uy, uz), pull)
    r0, r1, r2 = (lever[k] - turn[k] for k in range(3))
    i0 = 1.0 / h00
    l1 = h01 * i0
    l2 = h02 * i0
    d1 = h11 - l1 * h01
    e12 = h12 - l1 * h02
    d2 = h22 - l2 * h02
    y1 = r1 - l1 * r0
    y2 = r2 - l2 * r0
    i1 = 1.0 / d1
    m12 = e12 * i1
    w2 = (y2 - m12 * y1) / (d2 - m12 * e12)
    w1 = y1 * i1 - m12 * w2
    w0 = r0 * i0 - l1 * w1 - l2 * w2
    swing = cross(lin, (w0, w1, w2))
    shift = [jnp.where(fixed, 0.0, (swing[k] - pull[k]) * inverse) for k in range(3)]
    cx, cy, cz = (jnp.where(fixed, 0.0, 0.5 * w) for w in (w0, w1, w2))
    norm = cx * cx + cy * cy + cz * cz
    gain = 2.0 / (1.0 + norm)
    step = [
        [1.0 + gain * (cx * cx - norm), gain * (cx * cy - cz), gain * (cx * cz + cy)],
        [gain * (cx * cy + cz), 1.0 + gain * (cy * cy - norm), gain * (cy * cz - cx)],
        [gain * (cx * cz - cy), gain * (cy * cz + cx), 1.0 + gain * (cz * cz - norm)],
    ]
    out = []
    for i in range(3):
        for j in range(3):
            out.append(sum(step[i][k] * pose_rows[3 * k + j] for k in range(3)))
    for i in range(3):
        out.append(sum(step[i][k] * pose_rows[9 + k] for k in range(3)) + shift[i])
    return out


def send(out_ref, acc_ref, pairs_ref):
    first, second = scatter(acc_ref, pairs_ref, out_ref.shape[2])
    for home in range(out_ref.shape[0]):
        out_ref[home, :8, :] = first
        out_ref[home, 8:, :] = second


def first_kernel(live_ref, ids_ref, counts_ref, pose_ref, src_ref, tgt_ref, pairs_ref, out_ref, *work):
    scan_dev = out_ref.shape[2] // out_ref.shape[0]
    pitch = pose_ref.shape[0] // out_ref.shape[0]

    def pose_of(scan):
        home = lax.div(scan, jnp.int32(scan_dev))
        base = home * pitch + (scan - home * scan_dev) * 12
        return lambda k, r: pose_ref[base + (9 + r if k == 3 else 3 * r + k)]

    all_tasks(pose_of, (live_ref, ids_ref, counts_ref, src_ref, tgt_ref), work)
    send(out_ref, work[0], pairs_ref)


def receive(in_ref):
    first = in_ref[0, :8, :]
    second = in_ref[0, 8:, :]
    for home in range(1, in_ref.shape[0]):
        first = first + in_ref[home, :8, :]
        second = second + in_ref[home, 8:, :]
    return first, second


def new_poses(in_ref, rows_ref, gauge_ref):
    first, second = receive(in_ref)
    scans = in_ref.shape[2]
    fixed = lax.broadcasted_iota(jnp.int32, (1, scans), 1) == gauge_ref[0]
    return updated(first, second, [rows_ref[k : k + 1, :] for k in range(12)], fixed)


def second_kernel(live_ref, ids_ref, counts_ref, gauge_ref, in_ref, rows_ref, src_ref, tgt_ref, pairs_ref, out_ref, next_ref, *work):
    table_ref, sem = work[-2:]
    for k, new_row in enumerate(new_poses(in_ref, rows_ref, gauge_ref)):
        next_ref[k : k + 1, :] = new_row
    copy = pltpu.make_async_copy(next_ref, table_ref, sem)
    copy.start()
    copy.wait()

    def pose_of(scan):
        return lambda k, r: table_ref[9 + r if k == 3 else 3 * r + k, scan]

    all_tasks(pose_of, (live_ref, ids_ref, counts_ref, src_ref, tgt_ref), work[:-2])
    send(out_ref, work[0], pairs_ref)


def last_kernel(own_ref, gauge_ref, in_ref, rows_ref, out_ref):
    scans = in_ref.shape[2]
    rows = new_poses(in_ref, rows_ref, gauge_ref)
    block = jnp.concatenate(rows + [jnp.zeros((LANES - 12, scans), jnp.float32)], axis=0)
    block = pltpu.roll(block, scans - own_ref[0], 1)[:, :LANES]
    out_ref[...] = block.T[: out_ref.shape[0], :12]


def body(source_points, target_points, pair_scans, point_counts, live_tasks, pose_init, gauge):
    homes = lax.axis_size(AXES)
    scan_dev = pose_init.shape[0]
    scans = homes * scan_dev
    tasks, _, width = source_points.shape
    chunks = width // LANES
    smem = pl.BlockSpec(memory_space=pltpu.SMEM)
    vmem = pl.BlockSpec(memory_space=pltpu.VMEM)
    scratch = [
        pltpu.VMEM((32, LANES), jnp.float32),
        pltpu.VMEM((1, width), jnp.float32),
        pltpu.VMEM((tasks, 8, width), jnp.float32),
        pltpu.VMEM((tasks + 1, 32, width), jnp.bfloat16),
        pltpu.VMEM(((tasks + 1) * chunks, 16, LANES), jnp.bfloat16),
        pltpu.VMEM(((tasks + 1) * chunks, LANES, 32), jnp.bfloat16),
        pltpu.VMEM((tasks + 1, 16, width), jnp.float32),
        pltpu.VMEM((STEP, LANES, width), jnp.bfloat16),
        pltpu.VMEM((STEP, LANES, width), jnp.bfloat16),
        pltpu.SMEM((tasks * chunks + 4 * STEP,), jnp.int32),
    ]
    parts = jax.ShapeDtypeStruct((homes, 16, scans), jnp.float32)
    rows_shape = jax.ShapeDtypeStruct((12, scans), jnp.float32)
    swap = lambda value: lax.all_to_all(value, AXES, 0, 0, tiled=True)

    source = jnp.transpose(source_points, (1, 0, 2))
    target = jnp.transpose(target_points, (1, 0, 2))
    ids = pair_scans.T
    counts = point_counts.T
    pairs = jnp.pad(ids, ((0, 0), (0, LANES - tasks)), constant_values=-1)
    own = (lax.axis_index(AXES) * scan_dev).reshape(1).astype(jnp.int32)

    flat = scan_dev * 12
    pitch = -(-flat // LANES) * LANES
    mine = jnp.pad(pose_init.reshape(1, flat), ((0, 0), (0, pitch - flat)))
    poses = swap(jnp.broadcast_to(mine, (homes, pitch)))
    rows = poses[:, :flat].reshape(scans, 12).T
    sums = pl.pallas_call(
        first_kernel,
        out_shape=parts,
        in_specs=[smem] * 4 + [vmem] * 3,
        out_specs=vmem,
        scratch_shapes=scratch,
        name="terms_first",
    )(live_tasks, ids, counts, poses.reshape(-1), source, target, pairs)
    sums, rows = pl.pallas_call(
        second_kernel,
        out_shape=(parts, rows_shape),
        in_specs=[smem] * 4 + [vmem] * 5,
        out_specs=(vmem, vmem),
        scratch_shapes=scratch + [pltpu.SMEM((12, scans), jnp.float32), pltpu.SemaphoreType.DMA],
        name="terms_second",
    )(live_tasks, ids, counts, gauge, swap(sums), rows, source, target, pairs)
    return pl.pallas_call(
        last_kernel,
        out_shape=jax.ShapeDtypeStruct((scan_dev, 12), jnp.float32),
        in_specs=[smem] * 2 + [vmem] * 2,
        out_specs=vmem,
        name="update_last",
    )(own, gauge, swap(sums), rows)


def solution(mesh):
    spec = P(AXES, None)
    cube = P(AXES, None, None)
    return jax.shard_map(
        body,
        mesh=mesh,
        in_specs=(cube, cube, spec, spec, P(AXES), spec, P()),
        out_specs=spec,
        check_vma=False,
    )
```

```python
import jax
import jax.numpy as jnp
from jax import lax
from jax.experimental import pallas as pl
from jax.experimental.pallas import tpu as pltpu
from jax.sharding import PartitionSpec as P

AXES = ("gx", "gy", "gz")
ITERS = 2
SPREAD = 2.0
DAMPING = 1.0
FLOOR = -1e30
LOG2E = 1.4426950408889634
LIFT = 100.0
TINY = 2.0**-100
UNROLL = 8
STEP = 8
SCALE = 2.0 * SPREAD * LOG2E
LANES = 128
INNER_LIMIT = 1 << 20


def halves(value):
    first = value.astype(jnp.bfloat16).astype(jnp.float32)
    rest = value - first
    second = rest.astype(jnp.bfloat16).astype(jnp.float32)
    return first, second, rest - second


def moved(points_ref, task, pose, row3, width):
    reps = width // LANES

    def column(index):
        a, b, c = (pose(index, r) for r in range(3))
        col = jnp.where(row3 == 0, a, jnp.where(row3 == 1, b, c))
        return jnp.concatenate([col] * reps, axis=1)

    out = column(3)
    for axis in range(3):
        row = jnp.broadcast_to(points_ref[axis, pl.ds(task, 1), :], (8, width))
        out = out + column(axis) * row
    return out


def operands(task, pose_of, ids_ref, counts_ref, src_ref, tgt_ref):
    width = src_ref.shape[2]
    sub = lax.broadcasted_iota(jnp.int32, (8, LANES), 0)
    row3 = sub - 3 * (sub // 3)
    row = lax.broadcasted_iota(jnp.int32, (8, width), 0)
    lane = lax.broadcasted_iota(jnp.int32, (8, width), 1)
    pos_x = moved(src_ref, task, pose_of(ids_ref[0, task]), row3, width)
    pos_y = moved(tgt_ref, task, pose_of(ids_ref[1, task]), row3, width)
    sq_x = pos_x * pos_x
    norm_x = pltpu.roll(sq_x, 1, 0) + pltpu.roll(sq_x, 2, 0) + pltpu.roll(sq_x, 3, 0)
    base_x = jnp.where(row < 6, pos_x, jnp.where(row == 6, LIFT - SPREAD * LOG2E * norm_x, 1.0))
    sq_y = pos_y * pos_y
    norm_y = pltpu.roll(sq_y, 2, 0) + pltpu.roll(sq_y, 3, 0) + pltpu.roll(sq_y, 4, 0)
    last_y = jnp.where(lane < counts_ref[1, task], -SPREAD * LOG2E * norm_y, FLOOR)
    base_y = jnp.where(row < 6, SCALE * pos_y, jnp.where(row == 6, 1.0, last_y))
    x_one, x_two, x_three = halves(base_x)
    y_one, y_two, y_three = halves(base_y)
    low3 = row < 3
    mid3 = (row >= 3) & (row < 6)
    x_group = [
        x_one,
        jnp.where(low3 | (row == 7), x_one, x_three),
        jnp.where(row == 7, x_one, x_two),
    ]
    y_group = [
        jnp.where(mid3, y_two, y_one),
        jnp.where(low3 | (row == 7), y_three, y_one),
        jnp.where(low3 | (row == 6), y_one, y_two),
    ]
    blank = jnp.zeros((8, width), jnp.float32)
    mat_x = jnp.concatenate(x_group + [blank], axis=0).astype(jnp.bfloat16)
    mat_y = jnp.concatenate(y_group + [blank], axis=0).astype(jnp.bfloat16)
    return pos_x, mat_x, mat_y


def score_of(turned_y, mat_x):
    return jnp.dot(turned_y, mat_x, preferred_element_type=jnp.float32)


def pull_sums(mat_y, weight):
    return jnp.dot(mat_y, weight.astype(jnp.bfloat16), preferred_element_type=jnp.float32)


def moments(task, live, counts_ref, pos_x, sums, acc_ref, low_ref):
    width = pos_x.shape[1]
    row = lax.broadcasted_iota(jnp.int32, (8, width), 0)
    lane = lax.broadcasted_iota(jnp.int32, (8, width), 1)
    count_x = jnp.where(task < live, counts_ref[0, task], 0)
    top = sums[:8]
    bottom = sums[8:]
    total = top[6:7, :]
    valid = lane < count_x
    low3 = row < 3
    low_ref[...] = jnp.minimum(low_ref[...], jnp.where(valid[:1], total, 1.0))
    inverse = jnp.broadcast_to((1.0 / SCALE) / total, (8, width))
    match_mid = (top + bottom + pltpu.roll(bottom, 3, 0)) * inverse
    match = jnp.where(valid, jnp.where(low3, pltpu.roll(match_mid, 5, 0), match_mid), 0.0)
    pos = jnp.where(valid, pos_x, 0.0)
    diff = pos - match
    next_pos = pltpu.roll(pos, 7, 0)
    ones = jnp.where(valid & (row == 6), 1.0, 0.0)
    linear = jnp.where(low3, pos, jnp.where(row < 6, match, ones))
    turned = jnp.where(low3, next_pos, pltpu.roll(match, 2, 0))
    cross = pos * pltpu.roll(diff, 7, 0) - next_pos * diff
    tail = jnp.where(low3, cross, diff)
    acc_lane = lax.broadcasted_iota(jnp.int32, (8, LANES), 1)
    for slot, part in enumerate((linear, linear * linear, linear * turned, tail)):
        reduced = jnp.sum(part, axis=1, keepdims=True)
        span = pl.ds(8 * slot, 8)
        acc_ref[span, :] = jnp.where(acc_lane == task, reduced, acc_ref[span, :])


def all_tasks(pose_of, data, work):
    live_ref, ids_ref, counts_ref, src_ref, tgt_ref = data
    acc_ref, low_ref, pos_ref, mx_ref, my_ref, mt_ref, sums_ref, even_ref, odd_ref, items_ref = work
    tasks = src_ref.shape[1]
    width = src_ref.shape[2]
    chunks = width // LANES
    live = live_ref[0]
    acc_ref[...] = jnp.zeros_like(acc_ref)
    low_ref[...] = jnp.ones_like(low_ref)
    mx_ref[tasks] = jnp.zeros_like(mx_ref[tasks])
    for chunk in range(chunks):
        my_ref[tasks * chunks + chunk] = jnp.zeros_like(my_ref[0])
        mt_ref[tasks * chunks + chunk] = jnp.zeros_like(mt_ref[0])
    unroll = UNROLL if tasks % UNROLL == 0 else 1
    groups = (live + unroll - 1) // unroll
    def prepare(group, end):
        for inner in range(unroll):
            task = group * unroll + inner
            pos_x, mat_x, mat_y = operands(task, pose_of, ids_ref, counts_ref, src_ref, tgt_ref)
            pos_ref[task] = pos_x
            mx_ref[task] = mat_x
            for chunk in range(chunks):
                block = mat_y[:, chunk * LANES : (chunk + 1) * LANES]
                my_ref[task * chunks + chunk] = block[:16]
                mt_ref[task * chunks + chunk] = block.T
            for chunk in range(chunks):
                items_ref[end + chunk] = task * chunks + chunk
            used = (counts_ref[1, task] + LANES - 1) // LANES
            end = end + jnp.where(task < live, used, 0)
        return end

    count = lax.fori_loop(0, groups, prepare, jnp.int32(0))
    for pad in range(3 * STEP):
        items_ref[count + pad] = tasks * chunks
    rounds = (count + STEP - 1) // STEP

    def score(index, buffer_ref, slot):
        code = items_ref[index]
        score = score_of(mt_ref[code], mx_ref[code // chunks])
        buffer_ref[slot] = jnp.exp2(score).astype(jnp.bfloat16)

    def pull(index, buffer_ref, slot):
        code = items_ref[index]
        task = code // chunks
        out = pull_sums(my_ref[code], buffer_ref[slot])
        prior = jnp.where(code == task * chunks, 0.0, sums_ref[task])
        sums_ref[task] = prior + out

    def both(group, next_ref, this_ref):
        for slot in range(STEP):
            score((group + 1) * STEP + slot, next_ref, slot)
            pull(group * STEP + slot, this_ref, slot)

    for slot in range(STEP):
        score(slot, even_ref, slot)

    def pair(index, carry):
        both(2 * index, odd_ref, even_ref)

        @pl.when(2 * index + 1 < rounds)
        def _():
            both(2 * index + 1, even_ref, odd_ref)

        return carry

    lax.fori_loop(0, (rounds + 1) // 2, pair, 0)

    def finish(group, carry):
        for inner in range(unroll):
            task = group * unroll + inner
            moments(task, live, counts_ref, pos_ref[task], sums_ref[task], acc_ref, low_ref)
        return carry

    lax.fori_loop(0, groups, finish, 0)

    @pl.when(jnp.min(low_ref[...]) < TINY)
    def _():
        def again(task, carry):
            pos_x, mat_x, mat_y = operands(task, pose_of, ids_ref, counts_ref, src_ref, tgt_ref)
            score = score_of(mat_y.T, mat_x)
            weight = jnp.exp2(score - jnp.max(score, axis=0, keepdims=True))
            moments(task, live, counts_ref, pos_x, pull_sums(mat_y[:16], weight), acc_ref, low_ref)
            return carry

        lax.fori_loop(0, live, again, 0)


def scatter(acc_ref, pairs_ref, scans):
    row_id = lax.broadcasted_iota(jnp.int32, (scans, LANES), 0)
    parts = jnp.concatenate(halves(acc_ref[...]), axis=0).astype(jnp.bfloat16)

    def side(index):
        hot = (pairs_ref[index : index + 1, :] == row_id).astype(jnp.float32).astype(jnp.bfloat16)
        out = lax.dot_general(
            parts, hot, (((1,), (1,)), ((), ())), preferred_element_type=jnp.float32
        )
        return out[:32] + (out[32:64] + out[64:])

    sum_a = side(0)
    sum_b = side(1)
    row = lax.broadcasted_iota(jnp.int32, (8, scans), 0)

    def low(slot):
        span = slice(8 * slot, 8 * slot + 8)
        return sum_a[span] + pltpu.roll(sum_b[span], 5, 0)

    count = sum_a[:8] + sum_b[:8]
    mixed = low(2)
    tail = sum_a[24:] - sum_b[24:]
    first = jnp.where(row < 3, low(0), pltpu.roll(low(1), 3, 0))
    first = jnp.where(row < 6, first, jnp.where(row == 6, count, pltpu.roll(mixed, 7, 0)))
    second = jnp.where(row < 6, tail, pltpu.roll(mixed, 5, 0))
    return first, second


def updated(first, second, pose_rows, fixed):
    def cross(a, b):
        return (
            a[1] * b[2] - a[2] * b[1],
            a[2] * b[0] - a[0] * b[2],
            a[0] * b[1] - a[1] * b[0],
        )

    at = lambda arr, index: arr[index : index + 1, :]
    lin = [at(first, k) for k in range(3)]
    xx, yy, zz = (at(first, 3 + k) for k in range(3))
    mass = at(first, 6) + DAMPING
    xy = at(first, 7)
    yz = at(second, 6)
    zx = at(second, 7)
    turn = [at(second, 1), at(second, 2), at(second, 0)]
    pull = [at(second, 3 + k) for k in range(3)]
    inverse = 1.0 / mass
    sx, sy, sz = lin
    ux, uy, uz = sx * inverse, sy * inverse, sz * inverse
    h00 = (yy + zz) + DAMPING - (sy * uy + sz * uz)
    h11 = (xx + zz) + DAMPING - (sx * ux + sz * uz)
    h22 = (xx + yy) + DAMPING - (sx * ux + sy * uy)
    h01 = sx * uy - xy
    h02 = sx * uz - zx
    h12 = sy * uz - yz
    lever = cross((ux, uy, uz), pull)
    r0, r1, r2 = (lever[k] - turn[k] for k in range(3))
    i0 = 1.0 / h00
    l1 = h01 * i0
    l2 = h02 * i0
    d1 = h11 - l1 * h01
    e12 = h12 - l1 * h02
    d2 = h22 - l2 * h02
    y1 = r1 - l1 * r0
    y2 = r2 - l2 * r0
    i1 = 1.0 / d1
    m12 = e12 * i1
    w2 = (y2 - m12 * y1) / (d2 - m12 * e12)
    w1 = y1 * i1 - m12 * w2
    w0 = r0 * i0 - l1 * w1 - l2 * w2
    swing = cross(lin, (w0, w1, w2))
    shift = [jnp.where(fixed, 0.0, (swing[k] - pull[k]) * inverse) for k in range(3)]
    cx, cy, cz = (jnp.where(fixed, 0.0, 0.5 * w) for w in (w0, w1, w2))
    norm = cx * cx + cy * cy + cz * cz
    gain = 2.0 / (1.0 + norm)
    step = [
        [1.0 + gain * (cx * cx - norm), gain * (cx * cy - cz), gain * (cx * cz + cy)],
        [gain * (cx * cy + cz), 1.0 + gain * (cy * cy - norm), gain * (cy * cz - cx)],
        [gain * (cx * cz - cy), gain * (cy * cz + cx), 1.0 + gain * (cz * cz - norm)],
    ]
    out = []
    for i in range(3):
        for j in range(3):
            out.append(sum(step[i][k] * pose_rows[3 * k + j] for k in range(3)))
    for i in range(3):
        out.append(sum(step[i][k] * pose_rows[9 + k] for k in range(3)) + shift[i])
    return out


def send(out_ref, acc_ref, pairs_ref):
    first, second = scatter(acc_ref, pairs_ref, out_ref.shape[2])
    for home in range(out_ref.shape[0]):
        out_ref[home, :8, :] = first
        out_ref[home, 8:, :] = second


def first_kernel(live_ref, ids_ref, counts_ref, pose_ref, src_ref, tgt_ref, pairs_ref, out_ref, *work):
    scan_dev = out_ref.shape[2] // out_ref.shape[0]
    pitch = pose_ref.shape[0] // out_ref.shape[0]

    def pose_of(scan):
        home = lax.div(scan, jnp.int32(scan_dev))
        base = home * pitch + (scan - home * scan_dev) * 12
        return lambda k, r: pose_ref[base + (9 + r if k == 3 else 3 * r + k)]

    all_tasks(pose_of, (live_ref, ids_ref, counts_ref, src_ref, tgt_ref), work)
    send(out_ref, work[0], pairs_ref)


def receive(in_ref):
    first = in_ref[0, :8, :]
    second = in_ref[0, 8:, :]
    for home in range(1, in_ref.shape[0]):
        first = first + in_ref[home, :8, :]
        second = second + in_ref[home, 8:, :]
    return first, second


def new_poses(in_ref, rows_ref, gauge_ref):
    first, second = receive(in_ref)
    scans = in_ref.shape[2]
    fixed = lax.broadcasted_iota(jnp.int32, (1, scans), 1) == gauge_ref[0]
    return updated(first, second, [rows_ref[k : k + 1, :] for k in range(12)], fixed)


def second_kernel(live_ref, ids_ref, counts_ref, gauge_ref, in_ref, rows_ref, src_ref, tgt_ref, pairs_ref, out_ref, next_ref, *work):
    turn_ref, table_ref, sem = work[-3:]
    scans = in_ref.shape[2]
    homes = out_ref.shape[0]
    scan_dev = scans // homes
    for k, new_row in enumerate(new_poses(in_ref, rows_ref, gauge_ref)):
        next_ref[k : k + 1, :] = new_row
    copy = pltpu.make_async_copy(next_ref, table_ref, sem)
    copy.start()
    copy.wait()

    def pose_of(scan):
        return lambda k, r: table_ref[9 + r if k == 3 else 3 * r + k, scan]

    all_tasks(pose_of, (live_ref, ids_ref, counts_ref, src_ref, tgt_ref), work[:-3])
    first, second = scatter(work[0], pairs_ref, scans)
    blank = jnp.zeros((LANES - 16, scans), jnp.float32)
    turn_ref[...] = jnp.concatenate([first, second, blank], axis=0).T
    out = turn_ref[pl.ds(0, homes, stride=scan_dev), :]
    for local in range(1, scan_dev):
        out = out + pltpu.roll(turn_ref[pl.ds(local, homes, stride=scan_dev), :], 16 * local, 1)
    out_ref[...] = out


def last_kernel(own_ref, gauge_ref, in_ref, rows_ref, out_ref):
    scan_dev = out_ref.shape[0]
    scans = rows_ref.shape[1]
    blank = jnp.zeros((4, scans), jnp.float32)
    rows = jnp.concatenate([rows_ref[...], blank], axis=0)
    rows = pltpu.roll(rows, scans - own_ref[0], 1)[:, :LANES]
    total = jnp.sum(in_ref[...], axis=0, keepdims=True)
    turned = jnp.broadcast_to(total, (LANES, LANES)).T
    lane = lax.broadcasted_iota(jnp.int32, (8, LANES), 1)
    first = turned[:8]
    second = turned[8:16]
    for local in range(1, scan_dev):
        first = jnp.where(lane == local, turned[16 * local : 16 * local + 8], first)
        second = jnp.where(lane == local, turned[16 * local + 8 : 16 * local + 16], second)
    fixed = lane[:1] + own_ref[0] == gauge_ref[0]
    new = updated(first, second, [rows[k : k + 1] for k in range(12)], fixed)
    block = jnp.concatenate(new + [jnp.zeros((LANES - 12, LANES), jnp.float32)], axis=0)
    out_ref[...] = block.T[:scan_dev, :12]


def body(source_points, target_points, pair_scans, point_counts, live_tasks, pose_init, gauge):
    homes = lax.axis_size(AXES)
    scan_dev = pose_init.shape[0]
    scans = homes * scan_dev
    tasks, _, width = source_points.shape
    chunks = width // LANES
    smem = pl.BlockSpec(memory_space=pltpu.SMEM)
    vmem = pl.BlockSpec(memory_space=pltpu.VMEM)
    scratch = [
        pltpu.VMEM((32, LANES), jnp.float32),
        pltpu.VMEM((1, width), jnp.float32),
        pltpu.VMEM((tasks, 8, width), jnp.float32),
        pltpu.VMEM((tasks + 1, 32, width), jnp.bfloat16),
        pltpu.VMEM(((tasks + 1) * chunks, 16, LANES), jnp.bfloat16),
        pltpu.VMEM(((tasks + 1) * chunks, LANES, 32), jnp.bfloat16),
        pltpu.VMEM((tasks + 1, 16, width), jnp.float32),
        pltpu.VMEM((STEP, LANES, width), jnp.bfloat16),
        pltpu.VMEM((STEP, LANES, width), jnp.bfloat16),
        pltpu.SMEM((tasks * chunks + 4 * STEP,), jnp.int32),
    ]
    parts = jax.ShapeDtypeStruct((homes, 16, scans), jnp.float32)
    blocks = jax.ShapeDtypeStruct((homes, LANES), jnp.float32)
    rows_shape = jax.ShapeDtypeStruct((12, scans), jnp.float32)
    swap = lambda value: lax.all_to_all(value, AXES, 0, 0, tiled=True)

    ids = pair_scans.T
    counts = point_counts.T
    own = (lax.axis_index(AXES) * scan_dev).reshape(1).astype(jnp.int32)


    def inner(value):
        if value.size > INNER_LIMIT:
            return value
        return pltpu.with_memory_space_constraint(value, pltpu.VMEM)

    flat = scan_dev * 12
    pitch = -(-flat // LANES) * LANES
    mine = jnp.pad(pose_init.reshape(1, flat), ((0, 0), (0, pitch - flat)))
    source = jnp.transpose(source_points, (1, 0, 2))
    target = jnp.transpose(target_points, (1, 0, 2))
    pairs = inner(jnp.pad(ids, ((0, 0), (0, LANES - tasks)), constant_values=-1))
    poses = swap(jnp.broadcast_to(mine, (homes, pitch)))
    rows = poses[:, :flat].reshape(scans, 12).T
    sums = pl.pallas_call(
        first_kernel,
        out_shape=parts,
        in_specs=[smem] * 4 + [vmem] * 3,
        out_specs=vmem,
        scratch_shapes=scratch,
        name="terms_first",
    )(live_tasks, ids, counts, poses.reshape(-1), source, target, pairs)
    sums, rows = pl.pallas_call(
        second_kernel,
        out_shape=(blocks, rows_shape),
        in_specs=[smem] * 4 + [vmem] * 5,
        out_specs=(vmem, vmem),
        scratch_shapes=scratch
        + [
            pltpu.VMEM((scans, LANES), jnp.float32),
            pltpu.SMEM((12, scans), jnp.float32),
            pltpu.SemaphoreType.DMA,
        ],
        name="terms_second",
    )(live_tasks, ids, counts, gauge, inner(swap(sums)), inner(rows), source, target, pairs)
    return pl.pallas_call(
        last_kernel,
        out_shape=jax.ShapeDtypeStruct((scan_dev, 12), jnp.float32),
        in_specs=[smem] * 2 + [vmem] * 2,
        out_specs=vmem,
        name="update_last",
    )(own, gauge, inner(swap(sums)), inner(rows))


def solution(mesh):
    spec = P(AXES, None)
    cube = P(AXES, None, None)
    return jax.shard_map(
        body,
        mesh=mesh,
        in_specs=(cube, cube, spec, spec, P(AXES), spec, P()),
        out_specs=spec,
        check_vma=False,
    )
```

```python
import functools

import jax
import jax.numpy as jnp
from jax import lax
from jax.experimental import pallas as pl
from jax.experimental.pallas import tpu as pltpu
from jax.sharding import PartitionSpec as P

AXES = ("gx", "gy", "gz")
ITERS = 2
SPREAD = 2.0
DAMPING = 1.0
FLOOR = -1e30
LOG2E = 1.4426950408889634
LIFT = 100.0
TINY = 2.0**-100
ROWS = 24
STEP = 8
SCALE = 2.0 * SPREAD * LOG2E
LANES = 128
INNER_LIMIT = 1 << 20


def halves(value):
    first = value.astype(jnp.bfloat16).astype(jnp.float32)
    rest = value - first
    second = rest.astype(jnp.bfloat16).astype(jnp.float32)
    return first, second, rest - second


def score_of(turned_y, mat_x):
    return jnp.dot(turned_y, mat_x, preferred_element_type=jnp.float32)


def gather_columns(gathered, live, meta_ref, cols_ref):
    lane = lax.broadcasted_iota(jnp.int32, (1, LANES), 1)
    meta = meta_ref[...]
    count_x = jnp.where(lane < live, meta[2:3], 0).astype(jnp.float32)
    count_y = meta[3:4].astype(jnp.float32)
    ids = meta[:2].astype(jnp.float32)
    blank = jnp.zeros((LANES - 36, LANES), jnp.float32)
    parts = [gathered[:, :LANES], gathered[:, LANES:], count_x, count_y, ids, blank]
    cols_ref[...] = jnp.concatenate(parts, axis=0).T


def one_hot(values, rows):
    row = lax.broadcasted_iota(jnp.int32, (rows, values.shape[1]), 0)
    return jnp.where(row == values, 1.0, 0.0).astype(jnp.bfloat16)


def both_ids(meta_ref):
    meta = meta_ref[...]
    return jnp.concatenate([meta[0:1], meta[1:2]], axis=1)


def all_tasks(live_ref, counts_ref, src_ref, tgt_ref, work):
    cols_ref, vals_ref, low_ref, pos_ref, fx_ref, fy_ref, sums_ref = work[:7]
    even_ref, odd_ref, turn_even_ref, turn_odd_ref, items_ref, owner_ref = work[7:]
    tasks = src_ref.shape[1]
    width = src_ref.shape[2]
    chunks = width // LANES
    slots = tasks + 1
    live = live_ref[0]
    groups = (live + 7) // 8
    vals_ref[...] = jnp.zeros_like(vals_ref)
    low_ref[...] = jnp.ones_like(low_ref)
    for chunk in range(chunks):
        dead = pl.ds((chunk * slots + tasks) * ROWS, ROWS)
        fx_ref[dead, :] = jnp.zeros((ROWS, LANES), jnp.float32)
        fy_ref[dead, :] = jnp.zeros((ROWS, LANES), jnp.float32)
    lane_wide = lax.broadcasted_iota(jnp.int32, (8, width), 1).astype(jnp.float32)

    def prepare(group, end):
        base = pl.multiple_of(group * 8, 8)
        cols = cols_ref[pl.ds(base, 8), :]

        def place(points_ref, offset):
            raw = [points_ref[axis, pl.ds(base, 8), :] for axis in range(3)]
            out = []
            for r in range(3):
                value = cols[:, offset + 9 + r : offset + 10 + r]
                for axis in range(3):
                    entry = offset + 3 * r + axis
                    value = value + cols[:, entry : entry + 1] * raw[axis]
                out.append(value)
            return out, out[0] * out[0] + out[1] * out[1] + out[2] * out[2]

        pos, norm_x = place(src_ref, 0)
        for axis in range(3):
            pos_ref[axis, pl.ds(base, 8), :] = pos[axis]
        x_parts = [halves(value) for value in pos]
        n_parts = halves(LIFT - SPREAD * LOG2E * norm_x)
        pos_y, norm_y = place(tgt_ref, 16)
        inside = lane_wide < cols[:, 33:34]
        y_parts = [halves(SCALE * value) for value in pos_y]
        m_parts = halves(jnp.where(inside, -SPREAD * LOG2E * norm_y, FLOOR))
        one = jnp.ones((8, width), jnp.float32)
        pairs = []
        for first, second in ((0, 0), (0, 1), (0, 2)):
            pairs += [(x_parts[k][first], y_parts[k][second]) for k in range(3)]
        pairs += [(n_parts[k], one) for k in range(3)]
        pairs += [(x_parts[k][1], y_parts[k][0]) for k in range(3)]
        pairs += [(one, m_parts[0])]
        pairs += [(x_parts[k][1], y_parts[k][1]) for k in range(3)]
        pairs += [(x_parts[k][2], y_parts[k][0]) for k in range(3)]
        pairs += [(one, m_parts[1]), (one, m_parts[2])]
        for r, (left, right) in enumerate(pairs):
            for chunk in range(chunks):
                span = slice(chunk * LANES, (chunk + 1) * LANES)
                rows = pl.ds((chunk * slots + base) * ROWS + r, 8, stride=ROWS)
                fx_ref[rows, :] = left[:, span]
                fy_ref[rows, :] = right[:, span]
        for inner in range(8):
            task = jnp.minimum(base + inner, tasks - 1)
            for chunk in range(chunks):
                items_ref[end + chunk] = chunk * slots + task
                owner_ref[end + chunk] = task
            used = (counts_ref[1, task] + LANES - 1) // LANES
            end = end + jnp.where(base + inner < live, used, 0)
        return end

    for pad in range(STEP):
        items_ref[pad] = tasks
        owner_ref[pad] = tasks
    end = lax.fori_loop(0, groups, prepare, jnp.int32(STEP))

    def fill(pad, carry):
        items_ref[end + pad] = tasks
        owner_ref[end + pad] = tasks
        return carry

    lax.fori_loop(0, 3 * STEP, fill, 0)
    rounds = (end - 1) // STEP
    blank_x = jnp.zeros((32 - ROWS, width), jnp.float32)
    blank_y = jnp.zeros((32 - ROWS, LANES), jnp.float32)

    def factor_x(task):
        parts = [fx_ref[pl.ds((chunk * slots + task) * ROWS, ROWS), :] for chunk in range(chunks)]
        whole = jnp.concatenate([jnp.concatenate(parts, axis=1), blank_x], axis=0)
        return whole.astype(jnp.bfloat16)

    def turn_y(code):
        part = fy_ref[pl.ds(code * ROWS, ROWS), :]
        return jnp.concatenate([part, blank_y], axis=0).astype(jnp.bfloat16).T

    def pull_sums(code, weight):
        part = fy_ref[pl.ds(code * ROWS, 16), :].astype(jnp.bfloat16)
        return jnp.dot(part, weight, preferred_element_type=jnp.float32)

    def add_sums(task, out, first):
        for chunk in range(chunks):
            rows = pl.ds((chunk * slots + task) * 16, 16)
            part = out[:, chunk * LANES : (chunk + 1) * LANES]
            sums_ref[rows, :] = part + jnp.where(first, 0.0, sums_ref[rows, :])

    def turn(index, turned_ref, slot):
        turned_ref[slot] = turn_y(items_ref[index])

    def score(index, turned_ref, buffer_ref, slot):
        value = score_of(turned_ref[slot], factor_x(owner_ref[index]))
        buffer_ref[slot] = jnp.exp2(value).astype(jnp.bfloat16)

    def pull(index, buffer_ref, slot):
        code = items_ref[index]
        add_sums(owner_ref[index], pull_sums(code, buffer_ref[slot]), code <= tasks)

    def all_stages(group, this_ref, next_ref, turn_this_ref, turn_next_ref):
        for slot in range(STEP):
            score((group + 1) * STEP + slot, turn_next_ref, next_ref, slot)
            pull(group * STEP + slot, this_ref, slot)
            turn((group + 2) * STEP + slot, turn_this_ref, slot)

    for slot in range(STEP):
        turn(STEP + slot, turn_odd_ref, slot)

    def pair(index, carry):
        all_stages(2 * index, even_ref, odd_ref, turn_even_ref, turn_odd_ref)

        @pl.when(2 * index < rounds)
        def _():
            all_stages(2 * index + 1, odd_ref, even_ref, turn_odd_ref, turn_even_ref)

        return carry

    lax.fori_loop(0, rounds // 2 + 1, pair, 0)

    def finish(group):
        base = pl.multiple_of(group * 8, 8)
        cols = cols_ref[pl.ds(base, 8), :]
        lane = lax.broadcasted_iota(jnp.int32, (8, LANES), 1)
        totals = None
        for chunk in range(chunks):
            span = slice(chunk * LANES, (chunk + 1) * LANES)

            def row(index):
                rows = pl.ds((chunk * slots + base) * 16 + index, 8, stride=16)
                return sums_ref[rows, :]

            valid = lane_wide[:, span] < cols[:, 32:33]
            weight = row(9)
            low_ref[...] = jnp.minimum(low_ref[...], jnp.where(valid, weight, 1.0))
            inverse = (1.0 / SCALE) / weight
            match = []
            for k in range(3):
                value = (row(k) + row(3 + k) + row(6 + k)) * inverse
                match.append(jnp.where(valid, value, 0.0))
            pos = [jnp.where(valid, pos_ref[k, pl.ds(base, 8), span], 0.0) for k in range(3)]
            diff = [pos[k] - match[k] for k in range(3)]

            def shape(p):
                return [p[0], p[1], p[2], p[0] * p[0], p[1] * p[1], p[2] * p[2]]

            def mixed(p):
                return [p[0] * p[1], p[1] * p[2], p[2] * p[0]]

            values = shape(pos) + [jnp.where(valid, 1.0, 0.0)] + mixed(pos)[:1]
            values += list(cross(pos, diff)) + diff + mixed(pos)[1:]
            values += shape(match) + mixed(match)
            totals = values if totals is None else [p + q for p, q in zip(totals, values)]
        sums = [jnp.sum(value, axis=1, keepdims=True) for value in totals]
        order = sums[:16] + sums[16:22] + [sums[6], sums[22]]
        order += [-value for value in sums[8:14]] + sums[23:25]
        out = jnp.zeros((8, LANES), jnp.float32)
        for index, value in enumerate(order):
            out = jnp.where(lane == index, value, out)
        vals_ref[pl.ds(base, 8), :] = out

    def finish_all():
        def step(index, carry):
            for inner in range(wide):
                finish(index * wide + inner)
            return carry

        wide = 2 if tasks % 16 == 0 else 1
        lax.fori_loop(0, (groups + wide - 1) // wide, step, 0)

    finish_all()

    @pl.when(jnp.min(low_ref[...]) < TINY)
    def _():
        def again(task, carry):
            mat_x = factor_x(task)
            scores = [score_of(turn_y(chunk * slots + task), mat_x) for chunk in range(chunks)]
            top = jnp.max(scores[0], axis=0, keepdims=True)
            for value in scores[1:]:
                top = jnp.maximum(top, jnp.max(value, axis=0, keepdims=True))
            for chunk in range(chunks):
                weight = jnp.exp2(scores[chunk] - top).astype(jnp.bfloat16)
                add_sums(task, pull_sums(chunk * slots + task, weight), chunk == 0)
            return carry

        lax.fori_loop(0, live, again, 0)
        finish_all()


def pack(vals_ref, cols_ref, first_scan, tasks, scan_dev):
    sub = lax.broadcasted_iota(jnp.int32, (8, LANES), 0)
    lane = lax.broadcasted_iota(jnp.int32, (8, LANES), 1)
    tile = jnp.zeros((8, LANES), jnp.float32)
    own = [None] * scan_dev
    for group in range(tasks // 8):
        vals = vals_ref[8 * group : 8 * group + 8, :]
        cols = cols_ref[8 * group : 8 * group + 8, :]
        begin = 16 * group
        moved = pltpu.roll(vals, (begin - 16) % LANES, 1)
        tile = jnp.where((lane >= begin) & (lane < begin + 16), moved, tile)
        tile = jnp.where(lane == 80 + group, pltpu.roll(cols, 45 + group, 1), tile)
        for local in range(scan_dev):
            here = cols[:, 34:35] == (first_scan + local).astype(jnp.float32)
            part = jnp.where(here, vals, 0.0)
            own[local] = part if own[local] is None else own[local] + part
    sums = jnp.zeros((8, LANES), jnp.float32)
    for local in range(scan_dev):
        sums = jnp.where(sub == local, jnp.sum(own[local], axis=0, keepdims=True), sums)
    return jnp.where((lane >= 64) & (lane < 80), pltpu.roll(sums, 64, 1), tile)


def unpack(tiles, scans, groups, scan_dev):
    depth = tiles.shape[0]
    ids = tiles.T[80:88]
    spot = lax.broadcasted_iota(jnp.int32, (1, depth), 1)
    local = spot - 8 * (spot // 8)
    own = jnp.where(local < scan_dev, (spot // 8) * scan_dev + local, -1).astype(jnp.float32)
    row = lax.broadcasted_iota(jnp.int32, (scans, depth), 0).astype(jnp.float32)
    rows = [ids[group : group + 1] for group in range(groups)] + [own]
    hot = jnp.concatenate([jnp.where(row == ids_row, 1.0, 0.0) for ids_row in rows], axis=0)
    parts = jnp.concatenate(halves(tiles), axis=1).astype(jnp.bfloat16)
    out = jnp.dot(hot.astype(jnp.bfloat16), parts, preferred_element_type=jnp.float32)
    out = out[:, :LANES] + (out[:, LANES : 2 * LANES] + out[:, 2 * LANES :])
    total = out[:scans]
    for index in range(1, groups + 1):
        begin = 64 if index == groups else 16 * index
        total = total + pltpu.roll(out[index * scans : (index + 1) * scans], LANES - begin, 1)
    total = total.T
    return total[:8], total[8:16]


def scatter(vals_ref, hot_ref):
    vals = vals_ref[...]
    lane = lax.broadcasted_iota(jnp.int32, (LANES, LANES), 1)
    near = jnp.where(lane < 16, vals, 0.0)
    far = jnp.where(lane < 16, pltpu.roll(vals, LANES - 16, 1), 0.0)
    parts = jnp.concatenate(halves(jnp.concatenate([near, far], axis=0)), axis=1)
    out = jnp.dot(hot_ref[...], parts.astype(jnp.bfloat16), preferred_element_type=jnp.float32)
    return out[:, :LANES] + (out[:, LANES : 2 * LANES] + out[:, 2 * LANES :])


def cross(a, b):
    return (
        a[1] * b[2] - a[2] * b[1],
        a[2] * b[0] - a[0] * b[2],
        a[0] * b[1] - a[1] * b[0],
    )


def updated(first, second, pose_rows, fixed):
    at = lambda arr, index: arr[index : index + 1, :]
    lin = [at(first, k) for k in range(3)]
    xx, yy, zz = (at(first, 3 + k) for k in range(3))
    mass = at(first, 6) + DAMPING
    xy = at(first, 7)
    yz = at(second, 6)
    zx = at(second, 7)
    turn = [at(second, k) for k in range(3)]
    pull = [at(second, 3 + k) for k in range(3)]
    inverse = 1.0 / mass
    sx, sy, sz = lin
    ux, uy, uz = sx * inverse, sy * inverse, sz * inverse
    h00 = (yy + zz) + DAMPING - (sy * uy + sz * uz)
    h11 = (xx + zz) + DAMPING - (sx * ux + sz * uz)
    h22 = (xx + yy) + DAMPING - (sx * ux + sy * uy)
    h01 = sx * uy - xy
    h02 = sx * uz - zx
    h12 = sy * uz - yz
    lever = cross((ux, uy, uz), pull)
    r0, r1, r2 = (lever[k] - turn[k] for k in range(3))
    i0 = 1.0 / h00
    l1 = h01 * i0
    l2 = h02 * i0
    d1 = h11 - l1 * h01
    e12 = h12 - l1 * h02
    d2 = h22 - l2 * h02
    y1 = r1 - l1 * r0
    y2 = r2 - l2 * r0
    i1 = 1.0 / d1
    m12 = e12 * i1
    w2 = (y2 - m12 * y1) / (d2 - m12 * e12)
    w1 = y1 * i1 - m12 * w2
    w0 = r0 * i0 - l1 * w1 - l2 * w2
    swing = cross(lin, (w0, w1, w2))
    shift = [jnp.where(fixed, 0.0, (swing[k] - pull[k]) * inverse) for k in range(3)]
    cx, cy, cz = (jnp.where(fixed, 0.0, 0.5 * w) for w in (w0, w1, w2))
    norm = cx * cx + cy * cy + cz * cz
    gain = 2.0 / (1.0 + norm)
    step = [
        [1.0 + gain * (cx * cx - norm), gain * (cx * cy - cz), gain * (cx * cz + cy)],
        [gain * (cx * cy + cz), 1.0 + gain * (cy * cy - norm), gain * (cy * cz - cx)],
        [gain * (cx * cz - cy), gain * (cy * cz + cx), 1.0 + gain * (cz * cz - norm)],
    ]
    out = []
    for i in range(3):
        for j in range(3):
            out.append(sum(step[i][k] * pose_rows[3 * k + j] for k in range(3)))
    for i in range(3):
        out.append(sum(step[i][k] * pose_rows[9 + k] for k in range(3)) + shift[i])
    return out


def first_kernel(live_ref, counts_ref, own_ref, pose_ref, meta_ref, src_ref, tgt_ref, out_ref, *refs, scan_dev):
    hot_ref, work = refs[0], refs[1:]
    homes = out_ref.shape[0]
    ids = both_ids(meta_ref)
    home = lax.div(ids, jnp.int32(scan_dev))
    parts = jnp.concatenate(halves(pose_ref[...]), axis=1).astype(jnp.bfloat16)
    wide = lax.dot_general(
        parts,
        one_hot(jnp.where(ids < 0, -1, home), homes),
        (((0,), (0,)), ((), ())),
        preferred_element_type=jnp.float32,
    )
    pitch = pose_ref.shape[1]
    wide = wide[:pitch] + (wide[pitch : 2 * pitch] + wide[2 * pitch :])
    gathered = wide[:16]
    for local in range(1, scan_dev):
        here = ids - home * scan_dev == local
        gathered = jnp.where(here, wide[16 * local : 16 * local + 16], gathered)
    gather_columns(gathered, live_ref[0], meta_ref, work[0])
    all_tasks(live_ref, counts_ref, src_ref, tgt_ref, work)
    if out_ref.shape[1] == 8:
        total = pack(work[1], work[0], own_ref[0], src_ref.shape[1], scan_dev)
    else:
        hot_ref[...] = one_hot(ids, out_ref.shape[2])
        total = scatter(work[1], hot_ref).T[:16]
    for index in range(homes):
        out_ref[index] = total


def receive(in_ref):
    first = in_ref[0, :8, :]
    second = in_ref[0, 8:, :]
    for home in range(1, in_ref.shape[0]):
        first = first + in_ref[home, :8, :]
        second = second + in_ref[home, 8:, :]
    return first, second


def second_kernel(live_ref, counts_ref, gauge_ref, meta_ref, in_ref, rows_ref, src_ref, tgt_ref, out_ref, next_ref, *refs):
    hot_ref, work, turn_ref = refs[0], refs[1:-1], refs[-1]
    scans = rows_ref.shape[1]
    homes = out_ref.shape[0]
    scan_dev = scans // homes
    hot_ref[...] = one_hot(both_ids(meta_ref), scans)
    fixed = lax.broadcasted_iota(jnp.int32, (1, scans), 1) == gauge_ref[0]
    rows = [rows_ref[k : k + 1, :] for k in range(12)]
    if len(in_ref.shape) == 2:
        totals = unpack(in_ref[...], scans, src_ref.shape[1] // 8, scan_dev)
    else:
        totals = receive(in_ref)
    rows = updated(*totals, rows, fixed) + [jnp.zeros((4, scans), jnp.float32)]
    table = jnp.concatenate(rows, axis=0)
    next_ref[...] = table
    parts = jnp.concatenate(halves(table), axis=0).astype(jnp.bfloat16)
    wide = jnp.dot(parts, hot_ref[...], preferred_element_type=jnp.float32)
    gathered = wide[:16] + (wide[16:32] + wide[32:])
    gather_columns(gathered, live_ref[0], meta_ref, work[0])
    all_tasks(live_ref, counts_ref, src_ref, tgt_ref, work)
    turn_ref[...] = scatter(work[1], hot_ref)
    out = turn_ref[pl.ds(0, homes, stride=scan_dev), :]
    for local in range(1, scan_dev):
        out = out + pltpu.roll(turn_ref[pl.ds(local, homes, stride=scan_dev), :], 16 * local, 1)
    out_ref[...] = out


def last_kernel(own_ref, gauge_ref, in_ref, rows_ref, out_ref):
    scan_dev = out_ref.shape[0]
    scans = rows_ref.shape[1]
    rows = pltpu.roll(rows_ref[...], scans - own_ref[0], 1)[:, :LANES]
    total = jnp.sum(in_ref[...], axis=0, keepdims=True)
    turned = jnp.broadcast_to(total, (LANES, LANES)).T
    lane = lax.broadcasted_iota(jnp.int32, (8, LANES), 1)
    first = turned[:8]
    second = turned[8:16]
    for local in range(1, scan_dev):
        first = jnp.where(lane == local, turned[16 * local : 16 * local + 8], first)
        second = jnp.where(lane == local, turned[16 * local + 8 : 16 * local + 16], second)
    fixed = lane[:1] + own_ref[0] == gauge_ref[0]
    new = updated(first, second, [rows[k : k + 1] for k in range(12)], fixed)
    block = jnp.concatenate(new + [jnp.zeros((LANES - 12, LANES), jnp.float32)], axis=0)
    out_ref[...] = block.T[:scan_dev, :12]


def body(source_points, target_points, pair_scans, point_counts, live_tasks, pose_init, gauge):
    homes = lax.axis_size(AXES)
    scan_dev = pose_init.shape[0]
    scans = homes * scan_dev
    tasks, _, width = source_points.shape
    chunks = width // LANES
    slots = tasks + 1
    smem = pl.BlockSpec(memory_space=pltpu.SMEM)
    vmem = pl.BlockSpec(memory_space=pltpu.VMEM)
    scratch = [
        pltpu.VMEM((scans, 2 * LANES), jnp.bfloat16),
        pltpu.VMEM((LANES, LANES), jnp.float32),
        pltpu.VMEM((LANES, LANES), jnp.float32),
        pltpu.VMEM((8, LANES), jnp.float32),
        pltpu.VMEM((3, tasks, width), jnp.float32),
        pltpu.VMEM((chunks * slots * ROWS, LANES), jnp.float32),
        pltpu.VMEM((chunks * slots * ROWS, LANES), jnp.float32),
        pltpu.VMEM((chunks * slots * 16, LANES), jnp.float32),
        pltpu.VMEM((STEP, LANES, width), jnp.bfloat16),
        pltpu.VMEM((STEP, LANES, width), jnp.bfloat16),
        pltpu.VMEM((STEP, LANES, 32), jnp.bfloat16),
        pltpu.VMEM((STEP, LANES, 32), jnp.bfloat16),
        pltpu.SMEM((tasks * chunks + 6 * STEP,), jnp.int32),
        pltpu.SMEM((tasks * chunks + 6 * STEP,), jnp.int32),
    ]
    swap = lambda value: lax.all_to_all(value, AXES, 0, 0, tiled=True)

    def inner(value):
        if value.size > INNER_LIMIT:
            return value
        return pltpu.with_memory_space_constraint(value, pltpu.VMEM)

    flat = scan_dev * 16
    pitch = -(-flat // LANES) * LANES
    mine = jnp.pad(pose_init, ((0, 0), (0, 4))).reshape(1, flat)
    mine = jnp.pad(mine, ((0, 0), (0, pitch - flat)))
    source = jnp.transpose(source_points, (1, 0, 2))
    target = jnp.transpose(target_points, (1, 0, 2))
    counts = point_counts.T
    meta = jnp.concatenate([pair_scans.T, counts], axis=0)
    meta = inner(jnp.pad(meta, ((0, 0), (0, LANES - tasks)), constant_values=-1))
    own = (lax.axis_index(AXES) * scan_dev).reshape(1).astype(jnp.int32)
    poses = swap(jnp.broadcast_to(mine, (homes, pitch)))
    rows = poses[:, :flat].reshape(scans, 16).T
    packed = tasks <= 32 and tasks % 8 == 0 and scan_dev <= 8 and homes <= 64
    shape = (homes, 8, LANES) if packed else (homes, 16, scans)
    sums = pl.pallas_call(
        functools.partial(first_kernel, scan_dev=scan_dev),
        out_shape=jax.ShapeDtypeStruct(shape, jnp.float32),
        in_specs=[smem] * 3 + [vmem] * 4,
        out_specs=vmem,
        scratch_shapes=scratch,
        name="terms_first",
    )(live_tasks, counts, own, inner(poses), meta, source, target)
    sums = swap(sums)
    if packed:
        sums = sums.reshape(homes * 8, LANES)
    sums, rows = pl.pallas_call(
        second_kernel,
        out_shape=(
            jax.ShapeDtypeStruct((homes, LANES), jnp.float32),
            jax.ShapeDtypeStruct((16, scans), jnp.float32),
        ),
        in_specs=[smem] * 3 + [vmem] * 5,
        out_specs=(vmem, vmem),
        scratch_shapes=scratch + [pltpu.VMEM((scans, LANES), jnp.float32)],
        name="terms_second",
    )(live_tasks, counts, gauge, meta, inner(sums), inner(rows), source, target)
    return pl.pallas_call(
        last_kernel,
        out_shape=jax.ShapeDtypeStruct((scan_dev, 12), jnp.float32),
        in_specs=[smem] * 2 + [vmem] * 2,
        out_specs=vmem,
        name="update_last",
    )(own, gauge, inner(swap(sums)), inner(rows))


def solution(mesh):
    spec = P(AXES, None)
    cube = P(AXES, None, None)
    return jax.shard_map(
        body,
        mesh=mesh,
        in_specs=(cube, cube, spec, spec, P(AXES), spec, P()),
        out_specs=spec,
        check_vma=False,
    )
```

```python
import functools

import jax
import jax.numpy as jnp
from jax import lax
from jax.experimental import pallas as pl
from jax.experimental.pallas import tpu as pltpu
from jax.sharding import PartitionSpec as P

AXES = ("gx", "gy", "gz")
ITERS = 2
SPREAD = 2.0
DAMPING = 1.0
FLOOR = -1e30
LOG2E = 1.4426950408889634
LIFT = 100.0
TINY = 2.0**-100
ROWS = 24
STEP = 8
SCALE = 2.0 * SPREAD * LOG2E
LANES = 128
INNER_LIMIT = 1 << 20


def halves(value):
    first = value.astype(jnp.bfloat16).astype(jnp.float32)
    rest = value - first
    second = rest.astype(jnp.bfloat16).astype(jnp.float32)
    return first, second, rest - second


def score_of(turned_y, mat_x):
    return jnp.dot(turned_y, mat_x, preferred_element_type=jnp.float32)


def gather_columns(gathered, live, meta_ref, cols_ref):
    lane = lax.broadcasted_iota(jnp.int32, (1, LANES), 1)
    meta = meta_ref[...]
    count_x = jnp.where(lane < live, meta[2:3], 0).astype(jnp.float32)
    count_y = meta[3:4].astype(jnp.float32)
    ids = meta[:2].astype(jnp.float32)
    blank = jnp.zeros((LANES - 36, LANES), jnp.float32)
    parts = [gathered[:, :LANES], gathered[:, LANES:], count_x, count_y, ids, blank]
    cols_ref[...] = jnp.concatenate(parts, axis=0).T


def one_hot(values, rows):
    row = lax.broadcasted_iota(jnp.int32, (rows, values.shape[1]), 0)
    return jnp.where(row == values, 1.0, 0.0).astype(jnp.bfloat16)


def both_ids(meta_ref):
    meta = meta_ref[...]
    return jnp.concatenate([meta[0:1], meta[1:2]], axis=1)


def all_tasks(live_ref, counts_ref, src_ref, tgt_ref, work):
    cols_ref, vals_ref, low_ref, pos_ref, fx_ref, fy_ref, sums_ref = work[:7]
    even_ref, odd_ref, turn_even_ref, turn_odd_ref, items_ref, owner_ref = work[7:]
    tasks = src_ref.shape[1]
    width = src_ref.shape[2]
    chunks = width // LANES
    slots = tasks + 1
    live = live_ref[0]
    groups = (live + 7) // 8
    vals_ref[...] = jnp.zeros_like(vals_ref)
    low_ref[...] = jnp.ones_like(low_ref)
    for chunk in range(chunks):
        dead = pl.ds((chunk * slots + tasks) * ROWS, ROWS)
        fx_ref[dead, :] = jnp.zeros((ROWS, LANES), jnp.float32)
        fy_ref[dead, :] = jnp.zeros((ROWS, LANES), jnp.float32)
    lane_wide = lax.broadcasted_iota(jnp.int32, (8, width), 1).astype(jnp.float32)

    def prepare(group, end):
        base = pl.multiple_of(group * 8, 8)
        cols = cols_ref[pl.ds(base, 8), :]

        def place(points_ref, offset):
            raw = [points_ref[axis, pl.ds(base, 8), :] for axis in range(3)]
            out = []
            for r in range(3):
                value = cols[:, offset + 9 + r : offset + 10 + r]
                for axis in range(3):
                    entry = offset + 3 * r + axis
                    value = value + cols[:, entry : entry + 1] * raw[axis]
                out.append(value)
            return out, out[0] * out[0] + out[1] * out[1] + out[2] * out[2]

        pos, norm_x = place(src_ref, 0)
        for axis in range(3):
            pos_ref[axis, pl.ds(base, 8), :] = pos[axis]
        x_parts = [halves(value) for value in pos]
        n_parts = halves(LIFT - SPREAD * LOG2E * norm_x)
        pos_y, norm_y = place(tgt_ref, 16)
        inside = lane_wide < cols[:, 33:34]
        y_parts = [halves(SCALE * value) for value in pos_y]
        m_parts = halves(jnp.where(inside, -SPREAD * LOG2E * norm_y, FLOOR))
        one = jnp.ones((8, width), jnp.float32)
        left = [part[0] for part in x_parts] + [part[1] for part in x_parts]
        left += [n_parts[0], one] + [part[2] for part in x_parts]
        left += [n_parts[1], n_parts[2], one, one, one]
        right = [part[0] for part in y_parts] + [part[1] for part in y_parts]
        right += [one, m_parts[0]] + [part[2] for part in y_parts]
        right += [None, None, None, m_parts[2], m_parts[1]]
        for ref, values in ((fx_ref, left), (fy_ref, right)):
            for r, value in enumerate(values):
                if value is None:
                    continue
                for chunk in range(chunks):
                    span = slice(chunk * LANES, (chunk + 1) * LANES)
                    rows = pl.ds((chunk * slots + base) * ROWS + r, 8, stride=ROWS)
                    ref[rows, :] = value[:, span]
        for inner in range(8):
            task = jnp.minimum(base + inner, tasks - 1)
            for chunk in range(chunks):
                items_ref[end + chunk] = chunk * slots + task
                owner_ref[end + chunk] = task
            used = (counts_ref[1, task] + LANES - 1) // LANES
            end = end + jnp.where(base + inner < live, used, 0)
        return end

    for pad in range(STEP):
        items_ref[pad] = tasks
        owner_ref[pad] = tasks
    wide = 2 if tasks % 16 == 0 else 1

    def prepare_some(index, end):
        for inner in range(wide):
            end = prepare(index * wide + inner, end)
        return end

    steps = (groups + wide - 1) // wide
    end = lax.fori_loop(0, steps, prepare_some, jnp.int32(STEP))

    def fill(pad, carry):
        items_ref[end + pad] = tasks
        owner_ref[end + pad] = tasks
        return carry

    lax.fori_loop(0, 3 * STEP, fill, 0)
    rounds = (end - 1) // STEP
    sub = lax.broadcasted_iota(jnp.int32, (8, LANES), 0)

    def factor_x(task):
        parts = [fx_ref[pl.ds((chunk * slots + task) * ROWS, 16), :] for chunk in range(chunks)]
        whole = jnp.concatenate(parts, axis=1)
        main, rest = whole[:8], whole[8:]
        return jnp.concatenate([main, main, rest, main], axis=0).astype(jnp.bfloat16)

    def turn_y(code):
        part = fy_ref[pl.ds(code * ROWS, 16), :]
        main, rest = part[:8], part[8:]
        last = jnp.where(sub == 7, rest, 0.0)
        swapped = jnp.where(sub < 6, pltpu.roll(main, 3, 0), last)
        swapped = jnp.where(sub < 3, pltpu.roll(main, 5, 0), swapped)
        third = jnp.where(sub < 3, main, jnp.where(sub < 5, 1.0, 0.0))
        last = jnp.where(sub == 7, pltpu.roll(rest, 1, 0), 0.0)
        fourth = jnp.where(sub < 3, rest, last)
        whole = jnp.concatenate([main, swapped, third, fourth], axis=0)
        return whole.astype(jnp.bfloat16).T

    def pull_sums(code, weight):
        part = fy_ref[pl.ds(code * ROWS, 16), :].astype(jnp.bfloat16)
        return jnp.dot(part, weight, preferred_element_type=jnp.float32)

    def add_sums(task, out, first):
        for chunk in range(chunks):
            rows = pl.ds((chunk * slots + task) * ROWS, 16)
            part = out[:, chunk * LANES : (chunk + 1) * LANES]
            sums_ref[rows, :] = part + jnp.where(first, 0.0, sums_ref[rows, :])

    def turn(index, turned_ref, slot):
        turned_ref[slot] = turn_y(items_ref[index])

    def score(index, turned_ref, buffer_ref, slot):
        value = score_of(turned_ref[slot], factor_x(owner_ref[index]))
        buffer_ref[slot] = jnp.exp2(value).astype(jnp.bfloat16)

    def pull(index, buffer_ref, slot):
        code = items_ref[index]
        add_sums(owner_ref[index], pull_sums(code, buffer_ref[slot]), code <= tasks)

    def all_stages(group, this_ref, next_ref, turn_this_ref, turn_next_ref):
        for slot in range(STEP):
            score((group + 1) * STEP + slot, turn_next_ref, next_ref, slot)
            pull(group * STEP + slot, this_ref, slot)
            turn((group + 2) * STEP + slot, turn_this_ref, slot)

    for slot in range(STEP):
        turn(STEP + slot, turn_odd_ref, slot)

    def pair(index, carry):
        all_stages(2 * index, even_ref, odd_ref, turn_even_ref, turn_odd_ref)

        @pl.when(2 * index < rounds)
        def _():
            all_stages(2 * index + 1, odd_ref, even_ref, turn_odd_ref, turn_even_ref)

        return carry

    lax.fori_loop(0, rounds // 2 + 1, pair, 0)

    def finish(group):
        base = pl.multiple_of(group * 8, 8)
        cols = cols_ref[pl.ds(base, 8), :]
        lane = lax.broadcasted_iota(jnp.int32, (8, LANES), 1)
        totals = None
        for chunk in range(chunks):
            span = slice(chunk * LANES, (chunk + 1) * LANES)

            def row(index):
                rows = pl.ds((chunk * slots + base) * ROWS + index, 8, stride=ROWS)
                return sums_ref[rows, :]

            valid = lane_wide[:, span] < cols[:, 32:33]
            weight = row(6)
            low_ref[...] = jnp.minimum(low_ref[...], jnp.where(valid, weight, 1.0))
            inverse = (1.0 / SCALE) / weight
            match = []
            for k in range(3):
                value = (row(k) + row(3 + k) + row(8 + k)) * inverse
                match.append(jnp.where(valid, value, 0.0))
            pos = [jnp.where(valid, pos_ref[k, pl.ds(base, 8), span], 0.0) for k in range(3)]
            diff = [pos[k] - match[k] for k in range(3)]

            def shape(p):
                return [p[0], p[1], p[2], p[0] * p[0], p[1] * p[1], p[2] * p[2]]

            def mixed(p):
                return [p[0] * p[1], p[1] * p[2], p[2] * p[0]]

            values = shape(pos) + [jnp.where(valid, 1.0, 0.0)] + mixed(pos)[:1]
            values += list(cross(pos, diff)) + diff + mixed(pos)[1:]
            values += shape(match) + mixed(match)
            totals = values if totals is None else [p + q for p, q in zip(totals, values)]
        sums = [jnp.sum(value, axis=1, keepdims=True) for value in totals]
        order = sums[:16] + sums[16:22] + [sums[6], sums[22]]
        order += [-value for value in sums[8:14]] + sums[23:25]
        out = jnp.zeros((8, LANES), jnp.float32)
        for index, value in enumerate(order):
            out = jnp.where(lane == index, value, out)
        vals_ref[pl.ds(base, 8), :] = out

    def finish_all():
        def step(index, carry):
            for inner in range(wide):
                finish(index * wide + inner)
            return carry

        lax.fori_loop(0, steps, step, 0)

    finish_all()

    @pl.when(jnp.min(low_ref[...]) < TINY)
    def _():
        def again(task, carry):
            mat_x = factor_x(task)
            scores = [score_of(turn_y(chunk * slots + task), mat_x) for chunk in range(chunks)]
            top = jnp.max(scores[0], axis=0, keepdims=True)
            for value in scores[1:]:
                top = jnp.maximum(top, jnp.max(value, axis=0, keepdims=True))
            for chunk in range(chunks):
                weight = jnp.exp2(scores[chunk] - top).astype(jnp.bfloat16)
                add_sums(task, pull_sums(chunk * slots + task, weight), chunk == 0)
            return carry

        lax.fori_loop(0, live, again, 0)
        finish_all()


def pack(vals_ref, cols_ref, first_scan, tasks, scan_dev):
    sub = lax.broadcasted_iota(jnp.int32, (8, LANES), 0)
    lane = lax.broadcasted_iota(jnp.int32, (8, LANES), 1)
    tile = jnp.zeros((8, LANES), jnp.float32)
    own = [None] * scan_dev
    for group in range(tasks // 8):
        vals = vals_ref[8 * group : 8 * group + 8, :]
        cols = cols_ref[8 * group : 8 * group + 8, :]
        begin = 16 * group
        moved = pltpu.roll(vals, (begin - 16) % LANES, 1)
        tile = jnp.where((lane >= begin) & (lane < begin + 16), moved, tile)
        tile = jnp.where(lane == 80 + group, pltpu.roll(cols, 45 + group, 1), tile)
        for local in range(scan_dev):
            here = cols[:, 34:35] == (first_scan + local).astype(jnp.float32)
            part = jnp.where(here, vals, 0.0)
            own[local] = part if own[local] is None else own[local] + part
    sums = jnp.zeros((8, LANES), jnp.float32)
    for local in range(scan_dev):
        sums = jnp.where(sub == local, jnp.sum(own[local], axis=0, keepdims=True), sums)
    return jnp.where((lane >= 64) & (lane < 80), pltpu.roll(sums, 64, 1), tile)


def unpack(tiles, scans, groups, scan_dev):
    depth = tiles.shape[0]
    ids = tiles.T[80:88]
    spot = lax.broadcasted_iota(jnp.int32, (1, depth), 1)
    local = spot - 8 * (spot // 8)
    own = jnp.where(local < scan_dev, (spot // 8) * scan_dev + local, -1).astype(jnp.float32)
    row = lax.broadcasted_iota(jnp.int32, (scans, depth), 0).astype(jnp.float32)
    rows = [ids[group : group + 1] for group in range(groups)] + [own]
    hot = jnp.concatenate([jnp.where(row == ids_row, 1.0, 0.0) for ids_row in rows], axis=0)
    parts = jnp.concatenate(halves(tiles), axis=1).astype(jnp.bfloat16)
    out = jnp.dot(hot.astype(jnp.bfloat16), parts, preferred_element_type=jnp.float32)
    out = out[:, :LANES] + (out[:, LANES : 2 * LANES] + out[:, 2 * LANES :])
    total = out[:scans]
    for index in range(1, groups + 1):
        begin = 64 if index == groups else 16 * index
        total = total + pltpu.roll(out[index * scans : (index + 1) * scans], LANES - begin, 1)
    total = total.T
    return total[:8], total[8:16]


def scatter(vals_ref, hot_ref):
    vals = vals_ref[...]
    lane = lax.broadcasted_iota(jnp.int32, (LANES, LANES), 1)
    near = jnp.where(lane < 16, vals, 0.0)
    far = jnp.where(lane < 16, pltpu.roll(vals, LANES - 16, 1), 0.0)
    parts = jnp.concatenate(halves(jnp.concatenate([near, far], axis=0)), axis=1)
    out = jnp.dot(hot_ref[...], parts.astype(jnp.bfloat16), preferred_element_type=jnp.float32)
    return out[:, :LANES] + (out[:, LANES : 2 * LANES] + out[:, 2 * LANES :])


def cross(a, b):
    return (
        a[1] * b[2] - a[2] * b[1],
        a[2] * b[0] - a[0] * b[2],
        a[0] * b[1] - a[1] * b[0],
    )


def updated(first, second, pose_rows, fixed):
    at = lambda arr, index: arr[index : index + 1, :]
    lin = [at(first, k) for k in range(3)]
    xx, yy, zz = (at(first, 3 + k) for k in range(3))
    mass = at(first, 6) + DAMPING
    xy = at(first, 7)
    yz = at(second, 6)
    zx = at(second, 7)
    turn = [at(second, k) for k in range(3)]
    pull = [at(second, 3 + k) for k in range(3)]
    inverse = 1.0 / mass
    sx, sy, sz = lin
    ux, uy, uz = sx * inverse, sy * inverse, sz * inverse
    h00 = (yy + zz) + DAMPING - (sy * uy + sz * uz)
    h11 = (xx + zz) + DAMPING - (sx * ux + sz * uz)
    h22 = (xx + yy) + DAMPING - (sx * ux + sy * uy)
    h01 = sx * uy - xy
    h02 = sx * uz - zx
    h12 = sy * uz - yz
    lever = cross((ux, uy, uz), pull)
    r0, r1, r2 = (lever[k] - turn[k] for k in range(3))
    i0 = 1.0 / h00
    l1 = h01 * i0
    l2 = h02 * i0
    d1 = h11 - l1 * h01
    e12 = h12 - l1 * h02
    d2 = h22 - l2 * h02
    y1 = r1 - l1 * r0
    y2 = r2 - l2 * r0
    i1 = 1.0 / d1
    m12 = e12 * i1
    w2 = (y2 - m12 * y1) / (d2 - m12 * e12)
    w1 = y1 * i1 - m12 * w2
    w0 = r0 * i0 - l1 * w1 - l2 * w2
    swing = cross(lin, (w0, w1, w2))
    shift = [jnp.where(fixed, 0.0, (swing[k] - pull[k]) * inverse) for k in range(3)]
    cx, cy, cz = (jnp.where(fixed, 0.0, 0.5 * w) for w in (w0, w1, w2))
    norm = cx * cx + cy * cy + cz * cz
    gain = 2.0 / (1.0 + norm)
    step = [
        [1.0 + gain * (cx * cx - norm), gain * (cx * cy - cz), gain * (cx * cz + cy)],
        [gain * (cx * cy + cz), 1.0 + gain * (cy * cy - norm), gain * (cy * cz - cx)],
        [gain * (cx * cz - cy), gain * (cy * cz + cx), 1.0 + gain * (cz * cz - norm)],
    ]
    out = []
    for i in range(3):
        for j in range(3):
            out.append(sum(step[i][k] * pose_rows[3 * k + j] for k in range(3)))
    for i in range(3):
        out.append(sum(step[i][k] * pose_rows[9 + k] for k in range(3)) + shift[i])
    return out


def first_kernel(live_ref, counts_ref, own_ref, pose_ref, meta_ref, src_ref, tgt_ref, out_ref, *refs, scan_dev):
    hot_ref, work = refs[0], refs[1:]
    homes = out_ref.shape[0]
    ids = both_ids(meta_ref)
    home = lax.div(ids, jnp.int32(scan_dev))
    parts = jnp.concatenate(halves(pose_ref[...]), axis=1).astype(jnp.bfloat16)
    wide = lax.dot_general(
        parts,
        one_hot(jnp.where(ids < 0, -1, home), homes),
        (((0,), (0,)), ((), ())),
        preferred_element_type=jnp.float32,
    )
    pitch = pose_ref.shape[1]
    wide = wide[:pitch] + (wide[pitch : 2 * pitch] + wide[2 * pitch :])
    gathered = wide[:16]
    for local in range(1, scan_dev):
        here = ids - home * scan_dev == local
        gathered = jnp.where(here, wide[16 * local : 16 * local + 16], gathered)
    gather_columns(gathered, live_ref[0], meta_ref, work[0])
    all_tasks(live_ref, counts_ref, src_ref, tgt_ref, work)
    if out_ref.shape[1] == 8:
        total = pack(work[1], work[0], own_ref[0], src_ref.shape[1], scan_dev)
    else:
        hot_ref[...] = one_hot(ids, out_ref.shape[2])
        total = scatter(work[1], hot_ref).T[:16]
    for index in range(homes):
        out_ref[index] = total


def receive(in_ref):
    first = in_ref[0, :8, :]
    second = in_ref[0, 8:, :]
    for home in range(1, in_ref.shape[0]):
        first = first + in_ref[home, :8, :]
        second = second + in_ref[home, 8:, :]
    return first, second


def second_kernel(live_ref, counts_ref, gauge_ref, meta_ref, in_ref, rows_ref, src_ref, tgt_ref, out_ref, next_ref, *refs):
    hot_ref, work, turn_ref = refs[0], refs[1:-1], refs[-1]
    scans = rows_ref.shape[1]
    homes = out_ref.shape[0]
    scan_dev = scans // homes
    hot_ref[...] = one_hot(both_ids(meta_ref), scans)
    fixed = lax.broadcasted_iota(jnp.int32, (1, scans), 1) == gauge_ref[0]
    rows = [rows_ref[k : k + 1, :] for k in range(12)]
    if len(in_ref.shape) == 2:
        totals = unpack(in_ref[...], scans, src_ref.shape[1] // 8, scan_dev)
    else:
        totals = receive(in_ref)
    rows = updated(*totals, rows, fixed) + [jnp.zeros((4, scans), jnp.float32)]
    table = jnp.concatenate(rows, axis=0)
    next_ref[...] = table
    parts = jnp.concatenate(halves(table), axis=0).astype(jnp.bfloat16)
    wide = jnp.dot(parts, hot_ref[...], preferred_element_type=jnp.float32)
    gathered = wide[:16] + (wide[16:32] + wide[32:])
    gather_columns(gathered, live_ref[0], meta_ref, work[0])
    all_tasks(live_ref, counts_ref, src_ref, tgt_ref, work)
    turn_ref[...] = scatter(work[1], hot_ref)
    out = turn_ref[pl.ds(0, homes, stride=scan_dev), :]
    for local in range(1, scan_dev):
        out = out + pltpu.roll(turn_ref[pl.ds(local, homes, stride=scan_dev), :], 16 * local, 1)
    out_ref[...] = out


def last_kernel(own_ref, gauge_ref, in_ref, rows_ref, out_ref):
    scan_dev = out_ref.shape[0]
    scans = rows_ref.shape[1]
    rows = pltpu.roll(rows_ref[...], scans - own_ref[0], 1)[:, :LANES]
    total = jnp.sum(in_ref[...], axis=0, keepdims=True)
    turned = jnp.broadcast_to(total, (LANES, LANES)).T
    lane = lax.broadcasted_iota(jnp.int32, (8, LANES), 1)
    first = turned[:8]
    second = turned[8:16]
    for local in range(1, scan_dev):
        first = jnp.where(lane == local, turned[16 * local : 16 * local + 8], first)
        second = jnp.where(lane == local, turned[16 * local + 8 : 16 * local + 16], second)
    fixed = lane[:1] + own_ref[0] == gauge_ref[0]
    new = updated(first, second, [rows[k : k + 1] for k in range(12)], fixed)
    block = jnp.concatenate(new + [jnp.zeros((LANES - 12, LANES), jnp.float32)], axis=0)
    out_ref[...] = block.T[:scan_dev, :12]


def body(source_points, target_points, pair_scans, point_counts, live_tasks, pose_init, gauge):
    homes = lax.axis_size(AXES)
    scan_dev = pose_init.shape[0]
    scans = homes * scan_dev
    tasks, _, width = source_points.shape
    chunks = width // LANES
    slots = tasks + 1
    smem = pl.BlockSpec(memory_space=pltpu.SMEM)
    vmem = pl.BlockSpec(memory_space=pltpu.VMEM)
    scratch = [
        pltpu.VMEM((scans, 2 * LANES), jnp.bfloat16),
        pltpu.VMEM((LANES, LANES), jnp.float32),
        pltpu.VMEM((LANES, LANES), jnp.float32),
        pltpu.VMEM((8, LANES), jnp.float32),
        pltpu.VMEM((3, tasks, width), jnp.float32),
        pltpu.VMEM((chunks * slots * ROWS, LANES), jnp.float32),
        pltpu.VMEM((chunks * slots * ROWS, LANES), jnp.float32),
        pltpu.VMEM((chunks * slots * ROWS, LANES), jnp.float32),
        pltpu.VMEM((STEP, LANES, width), jnp.bfloat16),
        pltpu.VMEM((STEP, LANES, width), jnp.bfloat16),
        pltpu.VMEM((STEP, LANES, 32), jnp.bfloat16),
        pltpu.VMEM((STEP, LANES, 32), jnp.bfloat16),
        pltpu.SMEM((tasks * chunks + 6 * STEP,), jnp.int32),
        pltpu.SMEM((tasks * chunks + 6 * STEP,), jnp.int32),
    ]
    swap = lambda value: lax.all_to_all(value, AXES, 0, 0, tiled=True)

    def inner(value):
        if value.size > INNER_LIMIT:
            return value
        return pltpu.with_memory_space_constraint(value, pltpu.VMEM)

    flat = scan_dev * 16
    pitch = -(-flat // LANES) * LANES
    mine = jnp.pad(pose_init, ((0, 0), (0, 4))).reshape(1, flat)
    mine = jnp.pad(mine, ((0, 0), (0, pitch - flat)))
    source = jnp.transpose(source_points, (1, 0, 2))
    target = jnp.transpose(target_points, (1, 0, 2))
    counts = point_counts.T
    meta = jnp.concatenate([pair_scans.T, counts], axis=0)
    counts = pltpu.with_memory_space_constraint(counts, pltpu.SMEM)
    meta = inner(jnp.pad(meta, ((0, 0), (0, LANES - tasks)), constant_values=-1))
    own = (lax.axis_index(AXES) * scan_dev).reshape(1).astype(jnp.int32)
    poses = swap(jnp.broadcast_to(mine, (homes, pitch)))
    rows = poses[:, :flat].reshape(scans, 16).T
    packed = tasks <= 32 and tasks % 8 == 0 and scan_dev <= 8 and homes <= 64
    shape = (homes, 8, LANES) if packed else (homes, 16, scans)
    sums = pl.pallas_call(
        functools.partial(first_kernel, scan_dev=scan_dev),
        out_shape=jax.ShapeDtypeStruct(shape, jnp.float32),
        in_specs=[smem] * 3 + [vmem] * 4,
        out_specs=vmem,
        scratch_shapes=scratch,
        name="terms_first",
    )(live_tasks, counts, own, inner(poses), meta, source, target)
    sums = swap(sums)
    if packed:
        sums = sums.reshape(homes * 8, LANES)
    sums, rows = pl.pallas_call(
        second_kernel,
        out_shape=(
            jax.ShapeDtypeStruct((homes, LANES), jnp.float32),
            jax.ShapeDtypeStruct((16, scans), jnp.float32),
        ),
        in_specs=[smem] * 3 + [vmem] * 5,
        out_specs=(vmem, vmem),
        scratch_shapes=scratch + [pltpu.VMEM((scans, LANES), jnp.float32)],
        name="terms_second",
    )(live_tasks, counts, gauge, meta, inner(sums), inner(rows), source, target)
    return pl.pallas_call(
        last_kernel,
        out_shape=jax.ShapeDtypeStruct((scan_dev, 12), jnp.float32),
        in_specs=[smem] * 2 + [vmem] * 2,
        out_specs=vmem,
        name="update_last",
    )(own, gauge, inner(swap(sums)), inner(rows))


def solution(mesh):
    spec = P(AXES, None)
    cube = P(AXES, None, None)
    return jax.shard_map(
        body,
        mesh=mesh,
        in_specs=(cube, cube, spec, spec, P(AXES), spec, P()),
        out_specs=spec,
        check_vma=False,
    )
```

```python
import functools

import jax
import jax.numpy as jnp
from jax import lax
from jax.experimental import pallas as pl
from jax.experimental.pallas import tpu as pltpu
from jax.sharding import PartitionSpec as P

AXES = ("gx", "gy", "gz")
ITERS = 2
SPREAD = 2.0
DAMPING = 1.0
FLOOR = -1e30
LOG2E = 1.4426950408889634
LIFT = 100.0
TINY = 2.0**-100
ROWS = 24
STEP = 8
SCALE = 2.0 * SPREAD * LOG2E
LANES = 128
INNER_LIMIT = 1 << 20


def halves(value):
    first = value.astype(jnp.bfloat16).astype(jnp.float32)
    rest = value - first
    second = rest.astype(jnp.bfloat16).astype(jnp.float32)
    return first, second, rest - second


def score_of(turned_y, mat_x):
    return jnp.dot(turned_y, mat_x, preferred_element_type=jnp.float32)


def gather_columns(gathered, live, meta_ref, cols_ref):
    lane = lax.broadcasted_iota(jnp.int32, (1, LANES), 1)
    meta = meta_ref[...]
    count_x = jnp.where(lane < live, meta[2:3], 0).astype(jnp.float32)
    count_y = meta[3:4].astype(jnp.float32)
    ids = meta[:2].astype(jnp.float32)
    blank = jnp.zeros((LANES - 36, LANES), jnp.float32)
    parts = [gathered[:, :LANES], gathered[:, LANES:], count_x, count_y, ids, blank]
    cols_ref[...] = jnp.concatenate(parts, axis=0).T


def one_hot(values, rows):
    row = lax.broadcasted_iota(jnp.int32, (rows, values.shape[1]), 0)
    return jnp.where(row == values, 1.0, 0.0).astype(jnp.bfloat16)


def both_ids(meta_ref):
    meta = meta_ref[...]
    return jnp.concatenate([meta[0:1], meta[1:2]], axis=1)


def all_tasks(live_ref, counts_ref, src_ref, tgt_ref, work):
    cols_ref, vals_ref, low_ref, pos_ref, fx_ref, fy_ref, sums_ref = work[:7]
    even_ref, odd_ref, turn_even_ref, turn_odd_ref, items_ref, owner_ref = work[7:]
    tasks = src_ref.shape[1]
    width = src_ref.shape[2]
    chunks = width // LANES
    slots = tasks + 1
    live = live_ref[0]
    groups = (live + 7) // 8
    vals_ref[...] = jnp.zeros_like(vals_ref)
    low_ref[...] = jnp.ones_like(low_ref)
    for chunk in range(chunks):
        dead = pl.ds((chunk * slots + tasks) * ROWS, ROWS)
        fx_ref[dead, :] = jnp.zeros((ROWS, LANES), jnp.float32)
        fy_ref[dead, :] = jnp.zeros((ROWS, LANES), jnp.float32)
    lane_wide = lax.broadcasted_iota(jnp.int32, (8, width), 1).astype(jnp.float32)

    def prepare(group, end):
        base = pl.multiple_of(group * 8, 8)
        cols = cols_ref[pl.ds(base, 8), :]

        def place(points_ref, offset):
            raw = [points_ref[axis, pl.ds(base, 8), :] for axis in range(3)]
            out = []
            for r in range(3):
                value = cols[:, offset + 9 + r : offset + 10 + r]
                for axis in range(3):
                    entry = offset + 3 * r + axis
                    value = value + cols[:, entry : entry + 1] * raw[axis]
                out.append(value)
            return out, out[0] * out[0] + out[1] * out[1] + out[2] * out[2]

        pos, norm_x = place(src_ref, 0)
        for axis in range(3):
            pos_ref[axis, pl.ds(base, 8), :] = pos[axis]
        x_parts = [halves(value) for value in pos]
        n_parts = halves(LIFT - SPREAD * LOG2E * norm_x)
        pos_y, norm_y = place(tgt_ref, 16)
        inside = lane_wide < cols[:, 33:34]
        y_parts = [halves(SCALE * value) for value in pos_y]
        m_parts = halves(jnp.where(inside, -SPREAD * LOG2E * norm_y, FLOOR))
        one = jnp.ones((8, width), jnp.float32)
        left = [part[0] for part in x_parts] + [part[1] for part in x_parts]
        left += [n_parts[0], one] + [part[2] for part in x_parts]
        left += [n_parts[1], n_parts[2], one, one, one]
        right = [part[0] for part in y_parts] + [part[1] for part in y_parts]
        right += [one, m_parts[0]] + [part[2] for part in y_parts]
        right += [None, None, None, m_parts[2], m_parts[1]]
        for ref, values in ((fx_ref, left), (fy_ref, right)):
            for r, value in enumerate(values):
                if value is None:
                    continue
                for chunk in range(chunks):
                    span = slice(chunk * LANES, (chunk + 1) * LANES)
                    rows = pl.ds((chunk * slots + base) * ROWS + r, 8, stride=ROWS)
                    ref[rows, :] = value[:, span]
        for inner in range(8):
            task = jnp.minimum(base + inner, tasks - 1)
            for chunk in range(chunks):
                items_ref[end + chunk] = chunk * slots + task
                owner_ref[end + chunk] = task
            used = (counts_ref[1, task] + LANES - 1) // LANES
            end = end + jnp.where(base + inner < live, used, 0)
        return end

    for pad in range(STEP):
        items_ref[pad] = tasks
        owner_ref[pad] = tasks
    wide = 2 if tasks % 16 == 0 else 1

    def prepare_some(index, end):
        for inner in range(wide):
            end = prepare(index * wide + inner, end)
        return end

    steps = (groups + wide - 1) // wide
    end = lax.fori_loop(0, steps, prepare_some, jnp.int32(STEP))

    def fill(pad, carry):
        for inner in range(STEP):
            items_ref[end + pad * STEP + inner] = tasks
            owner_ref[end + pad * STEP + inner] = tasks
        return carry

    lax.fori_loop(0, 3, fill, 0)
    rounds = (end - 1) // STEP
    sub = lax.broadcasted_iota(jnp.int32, (8, LANES), 0)

    def factor_x(task):
        parts = [fx_ref[pl.ds((chunk * slots + task) * ROWS, 16), :] for chunk in range(chunks)]
        whole = jnp.concatenate(parts, axis=1)
        main, rest = whole[:8], whole[8:]
        return jnp.concatenate([main, main, rest, main], axis=0).astype(jnp.bfloat16)

    def turn_y(code):
        part = fy_ref[pl.ds(code * ROWS, 16), :]
        main, rest = part[:8], part[8:]
        last = jnp.where(sub == 7, rest, 0.0)
        swapped = jnp.where(sub < 6, pltpu.roll(main, 3, 0), last)
        swapped = jnp.where(sub < 3, pltpu.roll(main, 5, 0), swapped)
        third = jnp.where(sub < 3, main, jnp.where(sub < 5, 1.0, 0.0))
        last = jnp.where(sub == 7, pltpu.roll(rest, 1, 0), 0.0)
        fourth = jnp.where(sub < 3, rest, last)
        whole = jnp.concatenate([main, swapped, third, fourth], axis=0)
        return whole.astype(jnp.bfloat16).T

    def pull_sums(code, weight):
        part = fy_ref[pl.ds(code * ROWS, 16), :].astype(jnp.bfloat16)
        return jnp.dot(part, weight, preferred_element_type=jnp.float32)

    def add_sums(task, out, first):
        for chunk in range(chunks):
            rows = pl.ds((chunk * slots + task) * ROWS, 16)
            part = out[:, chunk * LANES : (chunk + 1) * LANES]
            sums_ref[rows, :] = part + jnp.where(first, 0.0, sums_ref[rows, :])

    def turn(index, turned_ref, slot):
        turned_ref[slot] = turn_y(items_ref[index])

    def score(index, turned_ref, buffer_ref, slot):
        value = score_of(turned_ref[slot], factor_x(owner_ref[index]))
        buffer_ref[slot] = jnp.exp2(value).astype(jnp.bfloat16)

    def pull(index, buffer_ref, slot):
        code = items_ref[index]
        add_sums(owner_ref[index], pull_sums(code, buffer_ref[slot]), code <= tasks)

    def all_stages(group, this_ref, next_ref, turn_this_ref, turn_next_ref):
        for slot in range(STEP):
            score((group + 1) * STEP + slot, turn_next_ref, next_ref, slot)
            pull(group * STEP + slot, this_ref, slot)
            turn((group + 2) * STEP + slot, turn_this_ref, slot)

    for slot in range(STEP):
        turn(STEP + slot, turn_odd_ref, slot)

    def pair(index, carry):
        all_stages(2 * index, even_ref, odd_ref, turn_even_ref, turn_odd_ref)

        @pl.when(2 * index < rounds)
        def _():
            all_stages(2 * index + 1, odd_ref, even_ref, turn_odd_ref, turn_even_ref)

        return carry

    lax.fori_loop(0, rounds // 2 + 1, pair, 0)

    def finish(group):
        base = pl.multiple_of(group * 8, 8)
        cols = cols_ref[pl.ds(base, 8), :]
        lane = lax.broadcasted_iota(jnp.int32, (8, LANES), 1)
        totals = None
        for chunk in range(chunks):
            span = slice(chunk * LANES, (chunk + 1) * LANES)

            def row(index):
                rows = pl.ds((chunk * slots + base) * ROWS + index, 8, stride=ROWS)
                return sums_ref[rows, :]

            valid = lane_wide[:, span] < cols[:, 32:33]
            weight = row(6)
            low_ref[...] = jnp.minimum(low_ref[...], jnp.where(valid, weight, 1.0))
            inverse = (1.0 / SCALE) / weight
            match = []
            for k in range(3):
                value = (row(k) + row(3 + k) + row(8 + k)) * inverse
                match.append(jnp.where(valid, value, 0.0))
            pos = [jnp.where(valid, pos_ref[k, pl.ds(base, 8), span], 0.0) for k in range(3)]
            diff = [pos[k] - match[k] for k in range(3)]

            def shape(p):
                return [p[0], p[1], p[2], p[0] * p[0], p[1] * p[1], p[2] * p[2]]

            def mixed(p):
                return [p[0] * p[1], p[1] * p[2], p[2] * p[0]]

            values = shape(pos) + [jnp.where(valid, 1.0, 0.0)] + mixed(pos)[:1]
            values += list(cross(pos, diff)) + diff + mixed(pos)[1:]
            values += shape(match) + mixed(match)
            totals = values if totals is None else [p + q for p, q in zip(totals, values)]
        sums = [jnp.sum(value, axis=1, keepdims=True) for value in totals]
        order = sums[:16] + sums[16:22] + [sums[6], sums[22]]
        order += [-value for value in sums[8:14]] + sums[23:25]
        out = jnp.zeros((8, LANES), jnp.float32)
        for index, value in enumerate(order):
            out = jnp.where(lane == index, value, out)
        vals_ref[pl.ds(base, 8), :] = out

    def finish_all():
        def step(index, carry):
            for inner in range(many):
                finish(index * many + inner)
            return carry

        many = 4 if tasks % 32 == 0 else wide
        lax.fori_loop(0, (groups + many - 1) // many, step, 0)

    finish_all()

    @pl.when(jnp.min(low_ref[...]) < TINY)
    def _():
        def again(task, carry):
            mat_x = factor_x(task)
            scores = [score_of(turn_y(chunk * slots + task), mat_x) for chunk in range(chunks)]
            top = jnp.max(scores[0], axis=0, keepdims=True)
            for value in scores[1:]:
                top = jnp.maximum(top, jnp.max(value, axis=0, keepdims=True))
            for chunk in range(chunks):
                weight = jnp.exp2(scores[chunk] - top).astype(jnp.bfloat16)
                add_sums(task, pull_sums(chunk * slots + task, weight), chunk == 0)
            return carry

        lax.fori_loop(0, live, again, 0)
        finish_all()


def pack(vals_ref, cols_ref, first_scan, tasks, scan_dev):
    sub = lax.broadcasted_iota(jnp.int32, (8, LANES), 0)
    lane = lax.broadcasted_iota(jnp.int32, (8, LANES), 1)
    tile = jnp.zeros((8, LANES), jnp.float32)
    own = [None] * scan_dev
    for group in range(tasks // 8):
        vals = vals_ref[8 * group : 8 * group + 8, :]
        cols = cols_ref[8 * group : 8 * group + 8, :]
        begin = 16 * group
        moved = pltpu.roll(vals, (begin - 16) % LANES, 1)
        tile = jnp.where((lane >= begin) & (lane < begin + 16), moved, tile)
        tile = jnp.where(lane == 80 + group, pltpu.roll(cols, 45 + group, 1), tile)
        for local in range(scan_dev):
            here = cols[:, 34:35] == (first_scan + local).astype(jnp.float32)
            part = jnp.where(here, vals, 0.0)
            own[local] = part if own[local] is None else own[local] + part
    sums = jnp.zeros((8, LANES), jnp.float32)
    for local in range(scan_dev):
        sums = jnp.where(sub == local, jnp.sum(own[local], axis=0, keepdims=True), sums)
    return jnp.where((lane >= 64) & (lane < 80), pltpu.roll(sums, 64, 1), tile)


def unpack(tiles, scans, groups, scan_dev):
    depth = tiles.shape[0]
    ids = tiles.T[80:88]
    spot = lax.broadcasted_iota(jnp.int32, (1, depth), 1)
    local = spot - 8 * (spot // 8)
    own = jnp.where(local < scan_dev, (spot // 8) * scan_dev + local, -1).astype(jnp.float32)
    row = lax.broadcasted_iota(jnp.int32, (scans, depth), 0).astype(jnp.float32)
    rows = [ids[group : group + 1] for group in range(groups)] + [own]
    hot = jnp.concatenate([jnp.where(row == ids_row, 1.0, 0.0) for ids_row in rows], axis=0)
    parts = jnp.concatenate(halves(tiles), axis=1).astype(jnp.bfloat16)
    out = jnp.dot(hot.astype(jnp.bfloat16), parts, preferred_element_type=jnp.float32)
    out = out[:, :LANES] + (out[:, LANES : 2 * LANES] + out[:, 2 * LANES :])
    total = out[:scans]
    for index in range(1, groups + 1):
        begin = 64 if index == groups else 16 * index
        total = total + pltpu.roll(out[index * scans : (index + 1) * scans], LANES - begin, 1)
    total = total.T
    return total[:8], total[8:16]


def scatter(vals_ref, hot_ref):
    vals = vals_ref[...]
    lane = lax.broadcasted_iota(jnp.int32, (LANES, LANES), 1)
    near = jnp.where(lane < 16, vals, 0.0)
    far = jnp.where(lane < 16, pltpu.roll(vals, LANES - 16, 1), 0.0)
    parts = jnp.concatenate(halves(jnp.concatenate([near, far], axis=0)), axis=1)
    out = jnp.dot(hot_ref[...], parts.astype(jnp.bfloat16), preferred_element_type=jnp.float32)
    return out[:, :LANES] + (out[:, LANES : 2 * LANES] + out[:, 2 * LANES :])


def cross(a, b):
    return (
        a[1] * b[2] - a[2] * b[1],
        a[2] * b[0] - a[0] * b[2],
        a[0] * b[1] - a[1] * b[0],
    )


def updated(first, second, pose_rows, fixed):
    at = lambda arr, index: arr[index : index + 1, :]
    lin = [at(first, k) for k in range(3)]
    xx, yy, zz = (at(first, 3 + k) for k in range(3))
    mass = at(first, 6) + DAMPING
    xy = at(first, 7)
    yz = at(second, 6)
    zx = at(second, 7)
    turn = [at(second, k) for k in range(3)]
    pull = [at(second, 3 + k) for k in range(3)]
    inverse = 1.0 / mass
    sx, sy, sz = lin
    ux, uy, uz = sx * inverse, sy * inverse, sz * inverse
    h00 = (yy + zz) + DAMPING - (sy * uy + sz * uz)
    h11 = (xx + zz) + DAMPING - (sx * ux + sz * uz)
    h22 = (xx + yy) + DAMPING - (sx * ux + sy * uy)
    h01 = sx * uy - xy
    h02 = sx * uz - zx
    h12 = sy * uz - yz
    lever = cross((ux, uy, uz), pull)
    r0, r1, r2 = (lever[k] - turn[k] for k in range(3))
    i0 = 1.0 / h00
    l1 = h01 * i0
    l2 = h02 * i0
    d1 = h11 - l1 * h01
    e12 = h12 - l1 * h02
    d2 = h22 - l2 * h02
    y1 = r1 - l1 * r0
    y2 = r2 - l2 * r0
    i1 = 1.0 / d1
    m12 = e12 * i1
    w2 = (y2 - m12 * y1) / (d2 - m12 * e12)
    w1 = y1 * i1 - m12 * w2
    w0 = r0 * i0 - l1 * w1 - l2 * w2
    swing = cross(lin, (w0, w1, w2))
    shift = [jnp.where(fixed, 0.0, (swing[k] - pull[k]) * inverse) for k in range(3)]
    cx, cy, cz = (jnp.where(fixed, 0.0, 0.5 * w) for w in (w0, w1, w2))
    norm = cx * cx + cy * cy + cz * cz
    gain = 2.0 / (1.0 + norm)
    step = [
        [1.0 + gain * (cx * cx - norm), gain * (cx * cy - cz), gain * (cx * cz + cy)],
        [gain * (cx * cy + cz), 1.0 + gain * (cy * cy - norm), gain * (cy * cz - cx)],
        [gain * (cx * cz - cy), gain * (cy * cz + cx), 1.0 + gain * (cz * cz - norm)],
    ]
    out = []
    for i in range(3):
        for j in range(3):
            out.append(sum(step[i][k] * pose_rows[3 * k + j] for k in range(3)))
    for i in range(3):
        out.append(sum(step[i][k] * pose_rows[9 + k] for k in range(3)) + shift[i])
    return out


def first_kernel(live_ref, counts_ref, own_ref, pose_ref, meta_ref, src_ref, tgt_ref, out_ref, *refs, scan_dev):
    hot_ref, work = refs[0], refs[1:]
    homes = out_ref.shape[0]
    ids = both_ids(meta_ref)
    home = lax.div(ids, jnp.int32(scan_dev))
    parts = jnp.concatenate(halves(pose_ref[...]), axis=1).astype(jnp.bfloat16)
    wide = lax.dot_general(
        parts,
        one_hot(jnp.where(ids < 0, -1, home), homes),
        (((0,), (0,)), ((), ())),
        preferred_element_type=jnp.float32,
    )
    pitch = pose_ref.shape[1]
    wide = wide[:pitch] + (wide[pitch : 2 * pitch] + wide[2 * pitch :])
    gathered = wide[:16]
    for local in range(1, scan_dev):
        here = ids - home * scan_dev == local
        gathered = jnp.where(here, wide[16 * local : 16 * local + 16], gathered)
    gather_columns(gathered, live_ref[0], meta_ref, work[0])
    all_tasks(live_ref, counts_ref, src_ref, tgt_ref, work)
    if out_ref.shape[1] == 8:
        total = pack(work[1], work[0], own_ref[0], src_ref.shape[1], scan_dev)
    else:
        hot_ref[...] = one_hot(ids, out_ref.shape[2])
        total = scatter(work[1], hot_ref).T[:16]
    for index in range(homes):
        out_ref[index] = total


def receive(in_ref):
    first = in_ref[0, :8, :]
    second = in_ref[0, 8:, :]
    for home in range(1, in_ref.shape[0]):
        first = first + in_ref[home, :8, :]
        second = second + in_ref[home, 8:, :]
    return first, second


def second_kernel(live_ref, counts_ref, gauge_ref, meta_ref, in_ref, rows_ref, src_ref, tgt_ref, out_ref, next_ref, *refs):
    hot_ref, work, turn_ref = refs[0], refs[1:-1], refs[-1]
    scans = rows_ref.shape[1]
    homes = out_ref.shape[0]
    scan_dev = scans // homes
    hot_ref[...] = one_hot(both_ids(meta_ref), scans)
    fixed = lax.broadcasted_iota(jnp.int32, (1, scans), 1) == gauge_ref[0]
    rows = [rows_ref[k : k + 1, :] for k in range(12)]
    if len(in_ref.shape) == 2:
        totals = unpack(in_ref[...], scans, src_ref.shape[1] // 8, scan_dev)
    else:
        totals = receive(in_ref)
    rows = updated(*totals, rows, fixed) + [jnp.zeros((4, scans), jnp.float32)]
    table = jnp.concatenate(rows, axis=0)
    next_ref[...] = table
    parts = jnp.concatenate(halves(table), axis=0).astype(jnp.bfloat16)
    wide = jnp.dot(parts, hot_ref[...], preferred_element_type=jnp.float32)
    gathered = wide[:16] + (wide[16:32] + wide[32:])
    gather_columns(gathered, live_ref[0], meta_ref, work[0])
    all_tasks(live_ref, counts_ref, src_ref, tgt_ref, work)
    turn_ref[...] = scatter(work[1], hot_ref)
    out = turn_ref[pl.ds(0, homes, stride=scan_dev), :]
    for local in range(1, scan_dev):
        out = out + pltpu.roll(turn_ref[pl.ds(local, homes, stride=scan_dev), :], 16 * local, 1)
    out_ref[...] = out


def last_kernel(own_ref, gauge_ref, in_ref, rows_ref, out_ref):
    scan_dev = out_ref.shape[0]
    scans = rows_ref.shape[1]
    rows = pltpu.roll(rows_ref[...], scans - own_ref[0], 1)[:, :LANES]
    total = jnp.sum(in_ref[...], axis=0, keepdims=True)
    turned = jnp.broadcast_to(total, (LANES, LANES)).T
    lane = lax.broadcasted_iota(jnp.int32, (8, LANES), 1)
    first = turned[:8]
    second = turned[8:16]
    for local in range(1, scan_dev):
        first = jnp.where(lane == local, turned[16 * local : 16 * local + 8], first)
        second = jnp.where(lane == local, turned[16 * local + 8 : 16 * local + 16], second)
    fixed = lane[:1] + own_ref[0] == gauge_ref[0]
    new = updated(first, second, [rows[k : k + 1] for k in range(12)], fixed)
    block = jnp.concatenate(new + [jnp.zeros((LANES - 12, LANES), jnp.float32)], axis=0)
    out_ref[...] = block.T[:scan_dev, :12]


def body(source_points, target_points, pair_scans, point_counts, live_tasks, pose_init, gauge):
    homes = lax.axis_size(AXES)
    scan_dev = pose_init.shape[0]
    scans = homes * scan_dev
    tasks, _, width = source_points.shape
    chunks = width // LANES
    slots = tasks + 1
    smem = pl.BlockSpec(memory_space=pltpu.SMEM)
    vmem = pl.BlockSpec(memory_space=pltpu.VMEM)
    scratch = [
        pltpu.VMEM((scans, 2 * LANES), jnp.bfloat16),
        pltpu.VMEM((LANES, LANES), jnp.float32),
        pltpu.VMEM((LANES, LANES), jnp.float32),
        pltpu.VMEM((8, LANES), jnp.float32),
        pltpu.VMEM((3, tasks, width), jnp.float32),
        pltpu.VMEM((chunks * slots * ROWS, LANES), jnp.float32),
        pltpu.VMEM((chunks * slots * ROWS, LANES), jnp.float32),
        pltpu.VMEM((chunks * slots * ROWS, LANES), jnp.float32),
        pltpu.VMEM((STEP, LANES, width), jnp.bfloat16),
        pltpu.VMEM((STEP, LANES, width), jnp.bfloat16),
        pltpu.VMEM((STEP, LANES, 32), jnp.bfloat16),
        pltpu.VMEM((STEP, LANES, 32), jnp.bfloat16),
        pltpu.SMEM((tasks * chunks + 6 * STEP,), jnp.int32),
        pltpu.SMEM((tasks * chunks + 6 * STEP,), jnp.int32),
    ]
    swap = lambda value: lax.all_to_all(value, AXES, 0, 0, tiled=True)

    def inner(value):
        if value.size > INNER_LIMIT:
            return value
        return pltpu.with_memory_space_constraint(value, pltpu.VMEM)

    flat = scan_dev * 16
    pitch = -(-flat // LANES) * LANES
    mine = jnp.pad(pose_init, ((0, 0), (0, 4))).reshape(1, flat)
    mine = jnp.pad(mine, ((0, 0), (0, pitch - flat)))
    source = jnp.transpose(source_points, (1, 0, 2))
    target = jnp.transpose(target_points, (1, 0, 2))
    counts = point_counts.T
    meta = jnp.concatenate([pair_scans.T, counts], axis=0)
    counts = pltpu.with_memory_space_constraint(counts, pltpu.SMEM)
    meta = inner(jnp.pad(meta, ((0, 0), (0, LANES - tasks)), constant_values=-1))
    own = (lax.axis_index(AXES) * scan_dev).reshape(1).astype(jnp.int32)
    poses = swap(jnp.broadcast_to(mine, (homes, pitch)))
    rows = poses[:, :flat].reshape(scans, 16).T
    packed = tasks <= 32 and tasks % 8 == 0 and scan_dev <= 8 and homes <= 64
    shape = (homes, 8, LANES) if packed else (homes, 16, scans)
    sums = pl.pallas_call(
        functools.partial(first_kernel, scan_dev=scan_dev),
        out_shape=jax.ShapeDtypeStruct(shape, jnp.float32),
        in_specs=[smem] * 3 + [vmem] * 4,
        out_specs=vmem,
        scratch_shapes=scratch,
        name="terms_first",
    )(live_tasks, counts, own, inner(poses), meta, source, target)
    sums = swap(sums)
    if packed:
        sums = sums.reshape(homes * 8, LANES)
    sums, rows = pl.pallas_call(
        second_kernel,
        out_shape=(
            jax.ShapeDtypeStruct((homes, LANES), jnp.float32),
            jax.ShapeDtypeStruct((16, scans), jnp.float32),
        ),
        in_specs=[smem] * 3 + [vmem] * 5,
        out_specs=(vmem, vmem),
        scratch_shapes=scratch + [pltpu.VMEM((scans, LANES), jnp.float32)],
        name="terms_second",
    )(live_tasks, counts, gauge, meta, inner(sums), inner(rows), source, target)
    return pl.pallas_call(
        last_kernel,
        out_shape=jax.ShapeDtypeStruct((scan_dev, 12), jnp.float32),
        in_specs=[smem] * 2 + [vmem] * 2,
        out_specs=vmem,
        name="update_last",
    )(own, gauge, inner(swap(sums)), inner(rows))


def solution(mesh):
    spec = P(AXES, None)
    cube = P(AXES, None, None)
    return jax.shard_map(
        body,
        mesh=mesh,
        in_specs=(cube, cube, spec, spec, P(AXES), spec, P()),
        out_specs=spec,
        check_vma=False,
    )
```
